128 devices in a mesh: rows: 16 (over z_hi, x, core), cols: 8 (over y, z_lo).
Axes of the slice: x: 4, y: 4, z: 4 (z_hi: 2, z_lo: 2; z = z_hi * 2 + z_lo), core: 2. Of those that a mesh axis runs over, the one named last changes fastest.
Arguments:
- block_values: bfloat16 [65536, 128], P(('rows', 'cols')), may hold values from -6 to 6
- block_length: int32 [65536], P(('rows', 'cols')), may hold values from 1 to 128
- block_owner: int32 [65536], P(('rows', 'cols')), may hold values from 0 to 16383, as said below
- block_second: int32 [65536], P(('rows', 'cols')), may hold values from 0 to 16383, as said below
- block_third: int32 [65536, 128], P(('rows', 'cols')), may hold values from 0 to 32767
- live_blocks: int32 [128], P(('rows', 'cols')), may hold values from 1 to 512, as said below
- second_factor: bfloat16 [16384, 256], P('cols', 'rows')
- third_factor: bfloat16 [32768, 256], P('cols', 'rows'), may hold values from -6 to 6
Outputs:
- first_factor: float32 [16384, 256], P('cols', 'rows')
The draws below stay inside these ranges and needn't reach their ends.
Inputs may be any that keep to these rules, and one draw needn't show every extreme that they name: `block_owner`: slot b lies on device d = b // 512 with index r along rows; its row lies in r * 16384 // 16 up to (r + 1) * 16384 // 16 - 1, the device's mode-1 slab. `block_second`: slot b lies on device d = b // 512 with index c along cols; its row lies in c * 16384 // 8 up to (c + 1) * 16384 // 8 - 1. `live_blocks`: some device uses all 512 slots in every draw.
All inputs are finite; a program needn't handle non-finite values.
Results may differ from the reference program's by a relative error of at most 0.0003.
Values may be sent and summed in bfloat16 or wider, within the bound.
No kernel may reach another device: no remote copies, remote signals or barrier semaphores. Data moves between devices by JAX's collectives and lax.ppermute only.
A program may use at most 128 MiB of HBM per device.

```python
import jax
import jax.numpy as jnp
from jax import lax

R = 256
L = 128
NB_DEV = 512
BLOCKS = 65536
I = 16384
J = 16384
K = 32768
N_ROWS = 16
N_COLS = 8
DEVICES = 128


def draw_block_owner(key, part):
    slot = jnp.arange(NB_DEV * DEVICES, dtype=jnp.int32)
    device = slot // NB_DEV
    slab = I // N_ROWS
    offset = jax.random.randint(key, (NB_DEV * DEVICES,), 0, slab, dtype=jnp.int32)
    return device // N_COLS * slab + offset


def draw_block_second(key, part):
    slot = jnp.arange(NB_DEV * DEVICES, dtype=jnp.int32)
    device = slot // NB_DEV
    span = J // N_COLS
    offset = jax.random.randint(jax.random.fold_in(key, 7), (NB_DEV * DEVICES,), 0, span, dtype=jnp.int32)
    return device % N_COLS * span + offset


def draw_live_blocks(key, part):
    first, second = jax.random.split(jax.random.fold_in(key, 11))
    counts = jax.random.randint(first, (DEVICES,), 1, NB_DEV + 1, dtype=jnp.int32)
    full = jax.random.randint(second, (), 0, DEVICES, dtype=jnp.int32)
    return jnp.where(jnp.arange(DEVICES, dtype=jnp.int32) == full, NB_DEV, counts)


def draw_second_factor(key, part):
    first = jax.random.fold_in(jax.random.fold_in(key, 13), 0)
    third = jax.random.fold_in(jax.random.fold_in(key, 13), 2)
    trend = 3.0 ** (jnp.arange(J, dtype=jnp.float32) / J)
    scale = trend * 10.0 ** jax.random.uniform(first, (J,), jnp.float32)
    base = jax.random.normal(third, (J, R), jnp.float32)
    return (scale[:, None] * base).astype(jnp.bfloat16)


def place_ends(drawn, stream_key, low, top_value):
    longest = drawn.shape.index(max(drawn.shape))
    spots = []
    for shift in (0, 1):
        where = [jax.random.randint(jax.random.fold_in(stream_key, axis), (), 0, length) for axis, length in enumerate(drawn.shape)]
        where[longest] = (where[longest] + shift) % drawn.shape[longest]
        spots.append(tuple(where))
    return drawn.at[spots[0]].set(low).at[spots[1]].set(top_value)


def steps_of(key, dims, cuts, smallest, high):
    gain = 1.0
    for dim, blocks in cuts:
        draws = jax.random.uniform(jax.random.fold_in(jax.random.fold_in(key, 6), dim), (blocks,), jnp.float32, smallest / len(cuts), high / len(cuts))
        gain = gain * jnp.repeat(jnp.exp(draws), dims[dim] // blocks).reshape((-1,) + (1,) * (len(dims) - 1 - dim))
    return gain


def scatter_about(own_key, dims, deviation, reach, shards=(), kind=jnp.bfloat16):
    values = jax.random.normal(own_key, dims, jnp.float32) * deviation
    if len(shards) > 0:
        values = steps_of(own_key, dims, shards, -0.22, 0.18) * values
    return jnp.clip(values, min=-reach, max=reach).astype(kind)


def setup_inputs(seed: int = 0) -> dict:
    key_of = jax.random.split(jax.random.key(seed), 9)
    return {
        "block_values": scatter_about(key_of[0], (BLOCKS, L), 1.0, 6.0, ((0, 128),)),
        "block_length": place_ends(jax.random.randint(key_of[1], (BLOCKS,), 1, L + 1), jax.random.fold_in(key_of[1], 1), 1, L).astype(jnp.int32),
        "block_owner": draw_block_owner(jax.random.fold_in(key_of[8], 71), 0),
        "block_second": draw_block_second(jax.random.fold_in(key_of[8], 71), 0),
        "block_third": place_ends(jax.random.randint(key_of[4], (BLOCKS, L), 0, K), jax.random.fold_in(key_of[4], 1), 0, K - 1).astype(jnp.int32),
        "live_blocks": draw_live_blocks(jax.random.fold_in(key_of[8], 71), 0),
        "second_factor": draw_second_factor(jax.random.fold_in(key_of[8], 71), 0),
        "third_factor": scatter_about(key_of[7], (K, R), 1.0, 6.0, ((0, 8), (1, 16))),
    }


def reference(block_values, block_length, block_owner, block_second, block_third, live_blocks, second_factor, third_factor):
    nblk = block_values.shape[0]
    width = block_values.shape[1]
    group = min(nblk, 512)
    position = jnp.arange(nblk, dtype=jnp.int32)
    live_block = position % NB_DEV < live_blocks[position // NB_DEV]
    lane = jnp.arange(width, dtype=jnp.int32)
    live = (lane[None, :] < block_length[:, None]) & live_block[:, None]
    masked = jnp.where(live, block_values, jnp.zeros((), jnp.bfloat16))
    steps = nblk // group

    def accumulate(total, pieces):
        values, third, second, owner = pieces
        rows = third_factor[third].astype(jnp.float32)
        fold = jnp.einsum('gt,gtr->gr', values.astype(jnp.float32), rows)
        contrib = second_factor[second].astype(jnp.float32) * fold
        return (total.at[owner].add(contrib), None)
    pieces = (masked.reshape(steps, group, width), block_third.reshape(steps, group, width), block_second.reshape(steps, group), block_owner.reshape(steps, group))
    start = jnp.zeros((I, R), jnp.float32)
    mttkrp, unused = lax.scan(accumulate, start, pieces)
    contract = (((0,), (0,)), ((), ()))
    gram_second = lax.dot_general(second_factor.astype(jnp.float32), second_factor.astype(jnp.float32), contract, preferred_element_type=jnp.float32) / J
    gram_third = lax.dot_general(third_factor.astype(jnp.float32), third_factor.astype(jnp.float32), contract, preferred_element_type=jnp.float32) / K
    gram = gram_second * gram_third
    factor = jnp.linalg.cholesky(gram)
    return jax.scipy.linalg.cho_solve((factor, True), mttkrp.T).T
```

```python
import functools

import jax
import jax.numpy as jnp
from jax import lax
from jax.experimental import pallas as pl
from jax.experimental.pallas import tpu as pltpu
from jax.sharding import PartitionSpec as P

BF = jnp.bfloat16
F32 = jnp.float32
NT = (((1,), (1,)), ((), ()))
NN = (((1,), (0,)), ((), ()))

LO = 256
HI = 128
NB = 16
PITCH = 24
STEP = 4


def dot(a, b, dims):
    return lax.dot_general(a, b, dims, preferred_element_type=F32)


def halves(x):
    head = x.astype(BF)
    return head, (x - head.astype(F32)).astype(BF)


def build_kernel(hi_ref, lo_ref, v_ref, head_ref, rest_ref, left, right):
    base = lax.broadcasted_iota(jnp.int32, (16, 128), 0)
    iota = [(base + 16 * j).astype(F32).astype(BF) for j in range(LO // 16)]
    one = jnp.ones((16, 128), BF)
    zero = jnp.zeros((16, 128), BF)
    for b in range(NB):
        hi, lo, v = (
            jnp.broadcast_to(ref[b : b + 1, :], (16, 128)).astype(BF)
            for ref in (hi_ref, lo_ref, v_ref)
        )
        a = jnp.concatenate([jnp.where(hi == iota[j], v, zero) for j in range(HI // 16)], 0)
        c = jnp.concatenate([jnp.where(lo == iota[j], one, zero) for j in range(LO // 16)], 0)
        s = dot(a, c, NT)
        left[pl.ds(b, HI, stride=PITCH), :] = s[:, :128]
        right[pl.ds(b, HI, stride=PITCH), :] = s[:, 128:]

    def split(i, carry):
        for u in range(4):
            h = i * 4 + u
            at = pl.multiple_of(h * PITCH, 8)
            x = jnp.concatenate([left[pl.ds(at, NB), :], right[pl.ds(at, NB), :]], 1)
            head_ref[h], rest_ref[h] = halves(x)
        return carry

    lax.fori_loop(0, HI // 4, split, 0)


def build(hi, lo, v):
    n = hi.shape[0]
    spec = pl.BlockSpec((NB, 128), lambda i: (i, 0))
    out = pl.BlockSpec((HI, NB, LO), lambda i: (0, i, 0))
    shape = jax.ShapeDtypeStruct((HI, n, LO), BF)
    return pl.pallas_call(
        build_kernel,
        grid=(n // NB,),
        in_specs=[spec] * 3,
        out_specs=[out, out],
        out_shape=[shape, shape],
        scratch_shapes=[pltpu.VMEM((HI * PITCH, 128), F32)] * 2,
        cost_estimate=pl.CostEstimate(
            flops=40_000_000_000, bytes_accessed=n * HI * LO * 4, transcendentals=0
        ),
    )(hi, lo, v)


def product_kernel(head_ref, rest_ref, t_ref, second_ref, owner_ref, part_ref, gram_ref, acc):
    step = pl.program_id(0)
    t = t_ref[...].reshape(256, STEP * LO)
    head = jnp.concatenate([head_ref[i] for i in range(STEP)], 1)
    rest = jnp.concatenate([rest_ref[i] for i in range(STEP)], 1)
    fold = dot(head, t, NT) + dot(rest, t, NT)
    gram = dot(t, t, NT)

    @pl.when(step == 0)
    def _():
        acc[...] = fold
        gram_ref[...] = gram

    @pl.when(step > 0)
    def _():
        acc[...] += fold
        gram_ref[...] += gram

    @pl.when(step == pl.num_programs(0) - 1)
    def _():
        head, rest = halves(second_ref[...].astype(F32) * acc[...])
        n = owner_ref.shape[1]
        slot = lax.broadcasted_iota(jnp.int32, (part_ref.shape[0], n), 0)
        hot = (slot == owner_ref[...]).astype(F32).astype(BF)
        part_ref[...] = dot(hot, head, NN) + dot(hot, rest, NN)


def product(head, rest, table, second, owner, slab):
    n = head.shape[1]
    s_spec = pl.BlockSpec((STEP, n, LO), lambda i: (i, 0, 0))
    per = table.shape[3] // (STEP * LO)
    return pl.pallas_call(
        product_kernel,
        grid=(HI // STEP,),
        in_specs=[
            s_spec,
            s_spec,
            pl.BlockSpec((16, 1, 16, STEP * LO), lambda i: (0, i // per, 0, i % per)),
            pl.BlockSpec((n, 256), lambda i: (0, 0)),
            pl.BlockSpec((1, n), lambda i: (0, 0)),
        ],
        out_specs=[
            pl.BlockSpec((slab, 256), lambda i: (0, 0)),
            pl.BlockSpec((256, 256), lambda i: (0, 0)),
        ],
        out_shape=[
            jax.ShapeDtypeStruct((slab, 256), F32),
            jax.ShapeDtypeStruct((256, 256), F32),
        ],
        scratch_shapes=[pltpu.VMEM((n, 256), F32)],
        cost_estimate=pl.CostEstimate(
            flops=30_000_000_000, bytes_accessed=100_000_000, transcendentals=0
        ),
    )(head, rest, table, second, owner)


def per_device(
    block_values,
    block_length,
    block_owner,
    block_second,
    block_third,
    live_blocks,
    second_factor,
    third_factor,
):
    n_rows = lax.axis_size("rows")
    n_cols = lax.axis_size("cols")
    row_at = lax.axis_index("rows")
    col_at = lax.axis_index("cols")
    nblk, width = block_values.shape
    range_rows = second_factor.shape[0]
    slab = range_rows * n_cols // n_rows

    second_range = lax.all_gather(second_factor, "rows", axis=1, tiled=True)
    third_part = lax.all_gather(third_factor.T, "cols")
    third_whole = lax.all_gather(third_part, "rows")

    contract = (((0,), (0,)), ((), ()))
    gram_second = lax.psum(dot(second_range, second_range, contract), "cols")

    lane = jnp.arange(width, dtype=jnp.int32)
    slot = jnp.arange(nblk, dtype=jnp.int32)
    live = (lane[None, :] < block_length[:, None]) & (slot < live_blocks[0])[:, None]
    values = jnp.where(live, block_values, jnp.zeros((), BF)).astype(F32)
    head, rest = build(
        (block_third // LO).astype(F32), (block_third % LO).astype(F32), values
    )
    picked = second_range[block_second - col_at * range_rows]
    owner = (block_owner - row_at * slab)[None, :]
    part, gram_third = product(head, rest, third_whole, picked, owner, slab)

    gram = (gram_second / (range_rows * n_cols)) * (
        gram_third / (third_factor.shape[0] * n_cols)
    )
    mine = lax.psum_scatter(part, "cols", scatter_dimension=0, tiled=True)
    factor = jnp.linalg.cholesky(gram)
    solved = jax.scipy.linalg.cho_solve((factor, True), mine.T).T
    moved = lax.all_to_all(
        lax.all_to_all(solved, "rows", split_axis=1, concat_axis=0, tiled=True),
        "cols",
        split_axis=0,
        concat_axis=0,
        tiled=True,
    )
    share = n_rows // n_cols
    owned_rows = mine.shape[0]
    reordered = moved.reshape(n_cols, share, owned_rows, moved.shape[1]).transpose(1, 0, 2, 3)
    return reordered.reshape(n_rows * owned_rows, moved.shape[1])


def solution(mesh):
    return jax.shard_map(
        per_device,
        mesh=mesh,
        in_specs=(
            P(("rows", "cols"), None),
            P(("rows", "cols")),
            P(("rows", "cols")),
            P(("rows", "cols")),
            P(("rows", "cols"), None),
            P(("rows", "cols")),
            P("cols", "rows"),
            P("cols", "rows"),
        ),
        out_specs=P("cols", "rows"),
        check_vma=False,
    )
```

```python
import jax
import jax.numpy as jnp
from jax import lax
from jax.experimental import pallas as pl
from jax.experimental.pallas import tpu as pltpu
from jax.sharding import PartitionSpec as P


BF = jnp.bfloat16
F32 = jnp.float32
NT = (((1,), (1,)), ((), ()))
NN = (((1,), (0,)), ((), ()))

LO = 256
HI = 128
NB = 16
PITCH = 24
PARTS = 4
STEP = 8
AXES = ("rows", "cols")
SHIFTS = (1, -1, 2)


def dot(a, b, dims):
    return lax.dot_general(a, b, dims, preferred_element_type=F32)


def halves(x):
    head = x.astype(BF)
    return head, (x - head.astype(F32)).astype(BF)


def build_kernel(hi_ref, lo_ref, v_ref, head_ref, rest_ref, left, right):
    base = lax.broadcasted_iota(jnp.int32, (16, 128), 0)
    iota = [(base + 16 * j).astype(F32).astype(BF) for j in range(LO // 16)]
    one = jnp.ones((16, 128), BF)
    zero = jnp.zeros((16, 128), BF)
    for b in range(NB):
        hi, lo, v = (
            jnp.broadcast_to(ref[b : b + 1, :], (16, 128)).astype(BF)
            for ref in (hi_ref, lo_ref, v_ref)
        )
        a = jnp.concatenate([jnp.where(hi == iota[j], v, zero) for j in range(HI // 16)], 0)
        c = jnp.concatenate([jnp.where(lo == iota[j], one, zero) for j in range(LO // 16)], 0)
        s = dot(a, c, NT)
        left[pl.ds(b, HI, stride=PITCH), :] = s[:, :128]
        right[pl.ds(b, HI, stride=PITCH), :] = s[:, 128:]

    def split(i, carry):
        for u in range(4):
            h = i * 4 + u
            at = pl.multiple_of(h * PITCH, 8)
            x = jnp.concatenate([left[pl.ds(at, NB), :], right[pl.ds(at, NB), :]], 1)
            head_ref[h], rest_ref[h] = halves(x)
        return carry

    lax.fori_loop(0, HI // 4, split, 0)


def build_more_kernel(hi_ref, lo_ref, v_ref, head_in, rest_in, *refs):
    build_kernel(hi_ref, lo_ref, v_ref, *refs)


def build(hi, lo, v):
    n = hi.shape[0]
    steps = n // NB // PARTS
    shape = jax.ShapeDtypeStruct((HI, n, LO), BF)
    made = ()
    for part in range(PARTS):
        spec = pl.BlockSpec((NB, 128), lambda i, at=part * steps: (at + i, 0))
        out = pl.BlockSpec((HI, NB, LO), lambda i, at=part * steps: (0, at + i, 0))
        call = pl.pallas_call(
            build_more_kernel if made else build_kernel,
            grid=(steps,),
            in_specs=[spec] * 3 + [pl.BlockSpec(memory_space=pl.ANY)] * len(made),
            out_specs=[out, out],
            out_shape=[shape, shape],
            scratch_shapes=[pltpu.VMEM((HI * PITCH, 128), F32)] * 2,
            input_output_aliases={3 + i: i for i in range(len(made))},
            cost_estimate=pl.CostEstimate(
                flops=40_000_000_000 // PARTS,
                bytes_accessed=n * HI * LO * 4 // PARTS,
                transcendentals=0,
            ),
        )
        made = call(hi, lo, v, *made)
    return made


def place(i):
    return {
        "x": i // 16 % 4,
        "y": i // 2 % 4,
        "z": i // 64 * 2 + i % 2,
        "core": i // 8 % 2,
    }


def device(at):
    return (((at["z"] // 2 * 4 + at["x"]) * 2 + at["core"]) * 4 + at["y"]) * 2 + at["z"] % 2


def shifted(value, dims, shift):
    pairs = []
    for i in range(128):
        at = place(i)
        dim = dims[at["core"]]
        at[dim] = (at[dim] + shift) % (2 if dim == "core" else 4)
        pairs.append((i, device(at)))
    return lax.ppermute(value, AXES, pairs)


def across(value):
    return shifted(value, ("core", "core"), 1)


def ring(value, dims):
    came = [value]
    for shift in SHIFTS:
        came.append(shifted(value, dims, shift))
    return jnp.concatenate(came, 0)


def gather_table(piece, core):
    half = piece.shape[1] // 2
    mine = lax.dynamic_slice_in_dim(piece, core * half, half, 1)
    other = lax.dynamic_slice_in_dim(piece, (1 - core) * half, half, 1)
    came = across(other)
    unit = jnp.where(core == 0, jnp.stack([mine, came]), jnp.stack([came, mine]))
    near = ring(unit[None], ("x", "y"))
    plane = ring(near[None], ("y", "z"))
    last = ("z", "x")
    left = shifted(plane, last, 1)
    right = shifted(plane, last, -1)
    far0 = shifted(left[:2], last, 1)
    far1 = shifted(right[2:], last, -1)
    own = [x.reshape(-1, *unit.shape) for x in (plane, left, right, far0, far1)]
    return own, [across(x) for x in own]


def piece_table(row_at, col_at, order):
    def spot(there, here):
        ahead = (there - here) & 3
        return jnp.where(ahead == 3, 1, jnp.where(ahead == 0, 0, ahead + 1))

    y, z_lo, z_hi, x = jnp.meshgrid(
        jnp.arange(4), jnp.arange(2), jnp.arange(2), jnp.arange(4), indexing="ij"
    )
    at_x = spot(x, row_at >> 1)
    at_y = spot(y, col_at >> 1)
    at_z = spot(z_hi * 2 + z_lo, (row_at >> 3) * 2 + (col_at & 1))
    first = jnp.where(order == 0, at_x, at_y)
    second = jnp.where(order == 0, at_y, at_z)
    third = jnp.where(order == 0, at_z, at_x)
    late = (third == 3) & (second >= 2)
    array = third + late
    index = (second - 2 * late) * 4 + first
    return jnp.concatenate([array.ravel(), index.ravel(), order[None]]).astype(jnp.int32)


def fetch(table, pieces, buf, sem, step, slot):
    n = buf.shape[1]
    for p in range(n):
        array = table[step * n + p]
        index = table[64 + step * n + p]
        for a, ref in enumerate(pieces):

            @pl.when(array == a)
            def _(ref=ref, p=p):
                pltpu.make_async_copy(ref.at[index], buf.at[slot, p], sem.at[slot]).start()


def accumulate(table, head_ref, rest_ref, pieces, fold_ref, gram_ref, buf, sem, begin):
    step = pl.program_id(0)
    slot = lax.rem(step, 2)

    @pl.when(step == 0)
    def _():
        begin()
        fetch(table, pieces, buf, sem, 0, 0)

    @pl.when(step + 1 < pl.num_programs(0))
    def _():
        fetch(table, pieces, buf, sem, step + 1, 1 - slot)

    pltpu.make_async_copy(pieces[0].at[pl.ds(0, buf.shape[1])], buf.at[slot], sem.at[slot]).wait()
    t = buf[slot].reshape(256, STEP * LO)
    head = jnp.concatenate([head_ref[i] for i in range(STEP)], 1)
    rest = jnp.concatenate([rest_ref[i] for i in range(STEP)], 1)
    fold_ref[...] += dot(head, t, NT) + dot(rest, t, NT)
    gram_ref[...] += dot(t, t, NT)


def first_kernel(table, head_ref, rest_ref, p0, p1, p2, p3, p4, fold_ref, gram_ref, buf, sem):
    def begin():
        fold_ref[...] = jnp.zeros_like(fold_ref)
        gram_ref[...] = jnp.zeros_like(gram_ref)

    accumulate(
        table, head_ref, rest_ref, (p0, p1, p2, p3, p4), fold_ref, gram_ref, buf, sem, begin
    )


def second_kernel(
    table, head_ref, rest_ref, p0, p1, p2, p3, p4,
    fold_in, gram_in, second_ref, owner_ref, part_ref, gram_ref, acc, buf, sem,
):
    def begin():
        acc[...] = fold_in[...]
        gram_ref[...] = gram_in[...]

    accumulate(table, head_ref, rest_ref, (p0, p1, p2, p3, p4), acc, gram_ref, buf, sem, begin)

    @pl.when(pl.program_id(0) == pl.num_programs(0) - 1)
    def _():
        head, rest = halves(second_ref[...].astype(F32) * acc[...])
        n = owner_ref.shape[1]
        slot = lax.broadcasted_iota(jnp.int32, (part_ref.shape[0], n), 0)
        hot = (slot == owner_ref[...]).astype(F32).astype(BF)
        part_ref[...] = dot(hot, head, NN) + dot(hot, rest, NN)


def product(table, head, rest, pieces, more, slab):
    n = head.shape[1]
    steps = HI // STEP // 2
    s_spec = pl.BlockSpec((STEP, n, LO), lambda i, table: (2 * i + table[128], 0, 0))
    any_spec = pl.BlockSpec(memory_space=pl.ANY)
    whole = lambda x: pl.BlockSpec(x.shape, lambda i, table: (0, 0))
    rows = slab if more else n
    out = [jax.ShapeDtypeStruct((rows, 256), F32), jax.ShapeDtypeStruct((256, 256), F32)]
    shape = pieces[0].shape
    scratch = [
        pltpu.VMEM((2, 8, *shape[1:]), BF),
        pltpu.SemaphoreType.DMA((2,)),
    ]
    if more:
        scratch = [pltpu.VMEM((n, 256), F32)] + scratch
    return pl.pallas_call(
        second_kernel if more else first_kernel,
        grid_spec=pltpu.PrefetchScalarGridSpec(
            num_scalar_prefetch=1,
            grid=(steps,),
            in_specs=[s_spec, s_spec] + [any_spec] * 5 + [whole(x) for x in more],
            out_specs=[whole(x) for x in out],
            scratch_shapes=scratch,
        ),
        out_shape=out,
        cost_estimate=pl.CostEstimate(
            flops=15_000_000_000, bytes_accessed=50_000_000, transcendentals=0
        ),
    )(table, head, rest, *pieces, *more)


def per_device(
    block_values,
    block_length,
    block_owner,
    block_second,
    block_third,
    live_blocks,
    second_factor,
    third_factor,
):
    n_rows = lax.axis_size("rows")
    n_cols = lax.axis_size("cols")
    row_at = lax.axis_index("rows")
    col_at = lax.axis_index("cols")
    nblk, width = block_values.shape
    range_rows = second_factor.shape[0]
    slab = range_rows * n_cols // n_rows

    second_range = lax.all_gather(second_factor, "rows", axis=1, tiled=True)
    core = row_at & 1
    own, swapped = gather_table(third_factor.T, core)

    contract = (((0,), (0,)), ((), ()))
    gram_second = lax.psum(dot(second_range, second_range, contract), "cols")

    lane = jnp.arange(width, dtype=jnp.int32)
    slot = jnp.arange(nblk, dtype=jnp.int32)
    live = (lane[None, :] < block_length[:, None]) & (slot < live_blocks[0])[:, None]
    values = jnp.where(live, block_values, jnp.zeros((), BF)).astype(F32)
    head, rest = build(
        (block_third // LO).astype(F32), (block_third % LO).astype(F32), values
    )
    picked = second_range[block_second - col_at * range_rows]
    owner = (block_owner - row_at * slab)[None, :]
    fold = product(piece_table(row_at, col_at, core), head, rest, own, (), slab)
    part, gram_third = product(
        piece_table(row_at, col_at, 1 - core), head, rest, swapped, (*fold, picked, owner), slab
    )

    gram = (gram_second / (range_rows * n_cols)) * (
        gram_third / (third_factor.shape[0] * n_cols)
    )
    spread = part.reshape(n_cols, slab // n_cols, -1)
    mine = jnp.sum(lax.all_to_all(spread, "cols", 0, 0, tiled=True), 0)
    factor = jnp.linalg.cholesky(gram)
    solved = jax.scipy.linalg.cho_solve((factor, True), mine.T).T
    moved = lax.all_to_all(
        lax.all_to_all(solved, "rows", split_axis=1, concat_axis=0, tiled=True),
        "cols",
        split_axis=0,
        concat_axis=0,
        tiled=True,
    )
    share = n_rows // n_cols
    owned_rows = mine.shape[0]
    reordered = moved.reshape(n_cols, share, owned_rows, moved.shape[1]).transpose(1, 0, 2, 3)
    return reordered.reshape(n_rows * owned_rows, moved.shape[1])


def solution(mesh):
    return jax.shard_map(
        per_device,
        mesh=mesh,
        in_specs=(
            P(("rows", "cols"), None),
            P(("rows", "cols")),
            P(("rows", "cols")),
            P(("rows", "cols")),
            P(("rows", "cols"), None),
            P(("rows", "cols")),
            P("cols", "rows"),
            P("cols", "rows"),
        ),
        out_specs=P("cols", "rows"),
        check_vma=False,
    )
```

```python
import jax
import jax.numpy as jnp
from jax import lax
from jax.experimental import pallas as pl
from jax.experimental.pallas import tpu as pltpu
from jax.sharding import PartitionSpec as P


BF = jnp.bfloat16
F32 = jnp.float32
NT = (((1,), (1,)), ((), ()))
NN = (((1,), (0,)), ((), ()))

LO = 256
HI = 128
NB = 16
PITCH = 24
PARTS = 4
STEP = 8
TOLERANCE = 3e-4
AXES = ("rows", "cols")
SHIFTS = (1, -1, 2)


def dot(a, b, dims):
    return lax.dot_general(a, b, dims, preferred_element_type=F32)


def halves(x):
    head = x.astype(BF)
    return head, (x - head.astype(F32)).astype(BF)


def build_kernel(hi_ref, lo_ref, v_ref, head_ref, rest_ref, left, right):
    base = lax.broadcasted_iota(jnp.int32, (16, 128), 0)
    iota = [(base + 16 * j).astype(F32).astype(BF) for j in range(LO // 16)]
    one = jnp.ones((16, 128), BF)
    zero = jnp.zeros((16, 128), BF)
    for b in range(NB):
        hi, lo, v = (
            jnp.broadcast_to(ref[b : b + 1, :], (16, 128)).astype(BF)
            for ref in (hi_ref, lo_ref, v_ref)
        )
        a = jnp.concatenate([jnp.where(hi == iota[j], v, zero) for j in range(HI // 16)], 0)
        c = jnp.concatenate([jnp.where(lo == iota[j], one, zero) for j in range(LO // 16)], 0)
        s = dot(a, c, NT)
        left[pl.ds(b, HI, stride=PITCH), :] = s[:, :128]
        right[pl.ds(b, HI, stride=PITCH), :] = s[:, 128:]

    def split(i, carry):
        for u in range(4):
            h = i * 4 + u
            at = pl.multiple_of(h * PITCH, 8)
            x = jnp.concatenate([left[pl.ds(at, NB), :], right[pl.ds(at, NB), :]], 1)
            head_ref[h], rest_ref[h] = halves(x)
        return carry

    lax.fori_loop(0, HI // 4, split, 0)


def build_more_kernel(hi_ref, lo_ref, v_ref, head_in, rest_in, *refs):
    build_kernel(hi_ref, lo_ref, v_ref, *refs)


def build(hi, lo, v):
    n = hi.shape[0]
    steps = n // NB // PARTS
    shape = jax.ShapeDtypeStruct((HI, n, LO), BF)
    made = ()
    for part in range(PARTS):
        spec = pl.BlockSpec((NB, 128), lambda i, at=part * steps: (at + i, 0))
        out = pl.BlockSpec((HI, NB, LO), lambda i, at=part * steps: (0, at + i, 0))
        call = pl.pallas_call(
            build_more_kernel if made else build_kernel,
            grid=(steps,),
            in_specs=[spec] * 3 + [pl.BlockSpec(memory_space=pl.ANY)] * len(made),
            out_specs=[out, out],
            out_shape=[shape, shape],
            scratch_shapes=[pltpu.VMEM((HI * PITCH, 128), F32)] * 2,
            input_output_aliases={3 + i: i for i in range(len(made))},
            cost_estimate=pl.CostEstimate(
                flops=40_000_000_000 // PARTS,
                bytes_accessed=n * HI * LO * 4 // PARTS,
                transcendentals=0,
            ),
        )
        made = call(hi, lo, v, *made)
    return made


def place(i):
    return {
        "x": i // 16 % 4,
        "y": i // 2 % 4,
        "z": i // 64 * 2 + i % 2,
        "core": i // 8 % 2,
    }


def device(at):
    return (((at["z"] // 2 * 4 + at["x"]) * 2 + at["core"]) * 4 + at["y"]) * 2 + at["z"] % 2


def shifted(value, dims, shift):
    pairs = []
    for i in range(128):
        at = place(i)
        dim = dims[at["core"]]
        at[dim] = (at[dim] + shift) % (2 if dim == "core" else 4)
        pairs.append((i, device(at)))
    return lax.ppermute(value, AXES, pairs)


def across(value):
    return shifted(value, ("core", "core"), 1)


def ring(value, dims):
    came = [value]
    for shift in SHIFTS:
        came.append(shifted(value, dims, shift))
    return jnp.concatenate(came, 0)


def gather_table(piece, core):
    half = piece.shape[1] // 2
    mine = lax.dynamic_slice_in_dim(piece, core * half, half, 1)
    other = lax.dynamic_slice_in_dim(piece, (1 - core) * half, half, 1)
    came = across(other)
    unit = jnp.where(core == 0, jnp.stack([mine, came]), jnp.stack([came, mine]))
    near = ring(unit[None], ("x", "y"))
    plane = ring(near[None], ("y", "z"))
    last = ("z", "x")
    left = shifted(plane, last, 1)
    right = shifted(plane, last, -1)
    far0 = shifted(left[:2], last, 1)
    far1 = shifted(right[2:], last, -1)
    own = [x.reshape(-1, *unit.shape) for x in (plane, left, right, far0, far1)]
    return own, [across(x) for x in own]


def piece_table(row_at, col_at, order):
    def spot(there, here):
        ahead = (there - here) & 3
        return jnp.where(ahead == 3, 1, jnp.where(ahead == 0, 0, ahead + 1))

    y, z_lo, z_hi, x = jnp.meshgrid(
        jnp.arange(4), jnp.arange(2), jnp.arange(2), jnp.arange(4), indexing="ij"
    )
    at_x = spot(x, row_at >> 1)
    at_y = spot(y, col_at >> 1)
    at_z = spot(z_hi * 2 + z_lo, (row_at >> 3) * 2 + (col_at & 1))
    first = jnp.where(order == 0, at_x, at_y)
    second = jnp.where(order == 0, at_y, at_z)
    third = jnp.where(order == 0, at_z, at_x)
    late = (third == 3) & (second >= 2)
    array = third + late
    index = (second - 2 * late) * 4 + first
    return jnp.concatenate([array.ravel(), index.ravel(), order[None]]).astype(jnp.int32)


def fetch(table, pieces, buf, sem, step, slot):
    n = buf.shape[1]
    for p in range(n):
        array = table[step * n + p]
        index = table[64 + step * n + p]
        for a, ref in enumerate(pieces):

            @pl.when(array == a)
            def _(ref=ref, p=p):
                pltpu.make_async_copy(ref.at[index], buf.at[slot, p], sem.at[slot]).start()


def accumulate(table, head_ref, rest_ref, pieces, fold_ref, gram_ref, buf, sem, begin):
    step = pl.program_id(0)
    slot = lax.rem(step, 2)

    @pl.when(step == 0)
    def _():
        begin()
        fetch(table, pieces, buf, sem, 0, 0)

    @pl.when(step + 1 < pl.num_programs(0))
    def _():
        fetch(table, pieces, buf, sem, step + 1, 1 - slot)

    pltpu.make_async_copy(pieces[0].at[pl.ds(0, buf.shape[1])], buf.at[slot], sem.at[slot]).wait()
    t = buf[slot].reshape(256, STEP * LO)
    head = jnp.concatenate([head_ref[i] for i in range(STEP)], 1)
    rest = jnp.concatenate([rest_ref[i] for i in range(STEP)], 1)
    fold_ref[...] += dot(head, t, NT) + dot(rest, t, NT)
    gram_ref[...] += dot(t, t, NT)


def first_kernel(table, head_ref, rest_ref, p0, p1, p2, p3, p4, fold_ref, gram_ref, buf, sem):
    def begin():
        fold_ref[...] = jnp.zeros_like(fold_ref)
        gram_ref[...] = jnp.zeros_like(gram_ref)

    accumulate(
        table, head_ref, rest_ref, (p0, p1, p2, p3, p4), fold_ref, gram_ref, buf, sem, begin
    )


def second_kernel(
    table, head_ref, rest_ref, p0, p1, p2, p3, p4,
    fold_in, gram_in, second_ref, owner_ref, part_ref, gram_ref, acc, buf, sem,
):
    def begin():
        acc[...] = fold_in[...]
        gram_ref[...] = gram_in[...]

    accumulate(table, head_ref, rest_ref, (p0, p1, p2, p3, p4), acc, gram_ref, buf, sem, begin)

    @pl.when(pl.program_id(0) == pl.num_programs(0) - 1)
    def _():
        head, rest = halves(second_ref[...].astype(F32) * acc[...])
        n = owner_ref.shape[1]
        slot = lax.broadcasted_iota(jnp.int32, (part_ref.shape[0], n), 0)
        hot = (slot == owner_ref[...]).astype(F32).astype(BF)
        part_ref[...] = dot(hot, head, NN) + dot(hot, rest, NN)


def product(table, head, rest, pieces, more, slab):
    n = head.shape[1]
    steps = HI // STEP // 2
    s_spec = pl.BlockSpec((STEP, n, LO), lambda i, table: (2 * i + table[128], 0, 0))
    any_spec = pl.BlockSpec(memory_space=pl.ANY)
    whole = lambda x: pl.BlockSpec(x.shape, lambda i, table: (0, 0))
    rows = slab if more else n
    out = [jax.ShapeDtypeStruct((rows, 256), F32), jax.ShapeDtypeStruct((256, 256), F32)]
    shape = pieces[0].shape
    scratch = [
        pltpu.VMEM((2, 8, *shape[1:]), BF),
        pltpu.SemaphoreType.DMA((2,)),
    ]
    if more:
        scratch = [pltpu.VMEM((n, 256), F32)] + scratch
    return pl.pallas_call(
        second_kernel if more else first_kernel,
        grid_spec=pltpu.PrefetchScalarGridSpec(
            num_scalar_prefetch=1,
            grid=(steps,),
            in_specs=[s_spec, s_spec] + [any_spec] * 5 + [whole(x) for x in more],
            out_specs=[whole(x) for x in out],
            scratch_shapes=scratch,
        ),
        out_shape=out,
        cost_estimate=pl.CostEstimate(
            flops=15_000_000_000, bytes_accessed=50_000_000, transcendentals=0
        ),
    )(table, head, rest, *pieces, *more)


def exact(a, b, dims):
    return lax.dot_general(a, b, dims, precision=lax.Precision.HIGHEST, preferred_element_type=F32)


def inverse_kernel(gram_ref, out_ref, ok_ref, a_ref, x_ref, r_ref):
    n = gram_ref.shape[0]
    at_row = lax.broadcasted_iota(jnp.int32, (n, n), 0)
    at_col = lax.broadcasted_iota(jnp.int32, (n, n), 1)
    eye = jnp.where(at_row == at_col, 1.0, 0.0)
    gram = gram_ref[...]
    diagonal = gram * eye
    by_row = lax.rsqrt(jnp.sum(diagonal, 1, keepdims=True))
    by_col = lax.rsqrt(jnp.sum(diagonal, 0, keepdims=True))
    a = gram * by_row * by_col
    bound = jnp.max(jnp.sum(jnp.abs(a), 0, keepdims=True))
    start = jnp.where(bound < 1.9, 1.0, 1.0 / bound)
    a_ref[...] = a
    x_ref[...] = start * eye
    r_ref[...] = eye - start * a

    def size(r):
        return jnp.sqrt(jnp.sum(r * r))

    def unfinished(state):
        i, now, before = state
        stuck = (now < 0.3) & (now > 0.5 * before)
        return (now > TOLERANCE) & (i < 40) & jnp.logical_not(stuck)

    def improve(state):
        i, now, _ = state
        x = x_ref[...] + exact(x_ref[...], r_ref[...], NN)
        r = eye - exact(a_ref[...], x, NN)
        x_ref[...] = x
        r_ref[...] = r
        return i + 1, size(r), now

    last = lax.while_loop(unfinished, improve, (0, size(r_ref[...]), jnp.float32(1e30)))
    x = x_ref[...] + exact(x_ref[...], r_ref[...], NN)
    out_ref[...] = x * by_row * by_col
    ok_ref[0] = jnp.where(last[1] <= TOLERANCE, 1, 0)


def inverse(gram):
    n = gram.shape[0]
    made, ok = pl.pallas_call(
        inverse_kernel,
        out_shape=[jax.ShapeDtypeStruct((n, n), F32), jax.ShapeDtypeStruct((1,), jnp.int32)],
        out_specs=[
            pl.BlockSpec(memory_space=pltpu.VMEM),
            pl.BlockSpec(memory_space=pltpu.SMEM),
        ],
        scratch_shapes=[pltpu.VMEM((n, n), F32)] * 3,
        cost_estimate=pl.CostEstimate(
            flops=5_000_000_000, bytes_accessed=600_000, transcendentals=0
        ),
    )(gram)

    def by_factor():
        factor = jnp.linalg.cholesky(gram)
        return jax.scipy.linalg.cho_solve((factor, True), jnp.eye(n, dtype=F32))

    return lax.cond(ok[0] == 1, lambda: made, by_factor)


def solve_kernel(inverse_ref, spread_ref, out_ref):
    total = spread_ref[0]
    for i in range(1, spread_ref.shape[0]):
        total = total + spread_ref[i]
    out_ref[...] = exact(inverse_ref[...], total, NT).reshape(out_ref.shape)


def solve(inverted, spread):
    n, rows = inverted.shape[0], spread.shape[1]
    return pl.pallas_call(
        solve_kernel,
        out_shape=jax.ShapeDtypeStruct((n // 16, 16, rows), F32),
        cost_estimate=pl.CostEstimate(
            flops=500_000_000, bytes_accessed=1_500_000, transcendentals=0
        ),
    )(inverted, spread)


def per_device(
    block_values,
    block_length,
    block_owner,
    block_second,
    block_third,
    live_blocks,
    second_factor,
    third_factor,
):
    n_rows = lax.axis_size("rows")
    n_cols = lax.axis_size("cols")
    row_at = lax.axis_index("rows")
    col_at = lax.axis_index("cols")
    nblk, width = block_values.shape
    range_rows = second_factor.shape[0]
    slab = range_rows * n_cols // n_rows

    second_range = lax.all_gather(second_factor, "rows", axis=1, tiled=True)
    core = row_at & 1
    own, swapped = gather_table(third_factor.T, core)

    contract = (((0,), (0,)), ((), ()))
    local_gram = dot(second_range, second_range, contract)
    gram_second = lax.psum(local_gram, "cols")

    lane = jnp.arange(width, dtype=jnp.int32)
    slot = jnp.arange(nblk, dtype=jnp.int32)
    live = (lane[None, :] < block_length[:, None]) & (slot < live_blocks[0])[:, None]
    values = jnp.where(live, block_values, jnp.zeros((), BF)).astype(F32)
    head, rest = build(
        (block_third // LO).astype(F32), (block_third % LO).astype(F32), values
    )
    picked = second_range[block_second - col_at * range_rows]
    owner = (block_owner - row_at * slab)[None, :]
    fold = product(piece_table(row_at, col_at, core), head, rest, own, (), slab)
    part, gram_third = product(
        piece_table(row_at, col_at, 1 - core), head, rest, swapped, (*fold, picked, owner), slab
    )

    gram = (gram_second / (range_rows * n_cols)) * (
        gram_third / (third_factor.shape[0] * n_cols)
    )
    spread = part.reshape(n_cols, slab // n_cols, -1)
    spread = lax.all_to_all(spread, "cols", 0, 0, tiled=True)
    solved = solve(inverse(gram), spread)
    moved = lax.all_to_all(solved, "rows", 0, 0, tiled=True)
    share = n_rows // n_cols
    moved = moved.reshape(n_cols, share, *solved.shape[1:])
    moved = lax.all_to_all(moved, "cols", 0, 0, tiled=True)
    return moved.transpose(1, 0, 3, 2).reshape(range_rows, solved.shape[1])


def solution(mesh):
    return jax.shard_map(
        per_device,
        mesh=mesh,
        in_specs=(
            P(("rows", "cols"), None),
            P(("rows", "cols")),
            P(("rows", "cols")),
            P(("rows", "cols")),
            P(("rows", "cols"), None),
            P(("rows", "cols")),
            P("cols", "rows"),
            P("cols", "rows"),
        ),
        out_specs=P("cols", "rows"),
        check_vma=False,
    )
```

```python
import jax
import jax.numpy as jnp
from jax import lax
from jax.experimental import pallas as pl
from jax.experimental.pallas import tpu as pltpu
from jax.sharding import PartitionSpec as P


BF = jnp.bfloat16
F32 = jnp.float32
NT = (((1,), (1,)), ((), ()))
NN = (((1,), (0,)), ((), ()))

LO = 256
HI = 128
NB = 16
PITCH = 24
PARTS = 4
STEP = 8
TOLERANCE = 3e-4
AXES = ("rows", "cols")
SHIFTS = (1, -1, 2)


def dot(a, b, dims):
    return lax.dot_general(a, b, dims, preferred_element_type=F32)


def halves(x):
    head = x.astype(BF)
    return head, (x - head.astype(F32)).astype(BF)


def build_kernel(hi_ref, lo_ref, v_ref, head_ref, rest_ref, left, right):
    base = lax.broadcasted_iota(jnp.int32, (16, 128), 0)
    iota = [(base + 16 * j).astype(F32).astype(BF) for j in range(LO // 16)]
    one = jnp.ones((16, 128), BF)
    zero = jnp.zeros((16, 128), BF)
    for b in range(NB):
        hi, lo, v = (
            jnp.broadcast_to(ref[b : b + 1, :], (16, 128)).astype(BF)
            for ref in (hi_ref, lo_ref, v_ref)
        )
        a = jnp.concatenate([jnp.where(hi == iota[j], v, zero) for j in range(HI // 16)], 0)
        c = jnp.concatenate([jnp.where(lo == iota[j], one, zero) for j in range(LO // 16)], 0)
        s = dot(a, c, NT)
        left[pl.ds(b, HI, stride=PITCH), :] = s[:, :128]
        right[pl.ds(b, HI, stride=PITCH), :] = s[:, 128:]

    def split(i, carry):
        for u in range(4):
            h = i * 4 + u
            at = pl.multiple_of(h * PITCH, 8)
            x = jnp.concatenate([left[pl.ds(at, NB), :], right[pl.ds(at, NB), :]], 1)
            head_ref[h], rest_ref[h] = halves(x)
        return carry

    lax.fori_loop(0, HI // 4, split, 0)


def build_more_kernel(hi_ref, lo_ref, v_ref, head_in, rest_in, *refs):
    build_kernel(hi_ref, lo_ref, v_ref, *refs)


def build(hi, lo, v):
    n = hi.shape[0]
    steps = n // NB // PARTS
    shape = jax.ShapeDtypeStruct((HI, n, LO), BF)
    made = ()
    for part in range(PARTS):
        spec = pl.BlockSpec((NB, 128), lambda i, at=part * steps: (at + i, 0))
        out = pl.BlockSpec((HI, NB, LO), lambda i, at=part * steps: (0, at + i, 0))
        call = pl.pallas_call(
            build_more_kernel if made else build_kernel,
            grid=(steps,),
            in_specs=[spec] * 3 + [pl.BlockSpec(memory_space=pl.ANY)] * len(made),
            out_specs=[out, out],
            out_shape=[shape, shape],
            scratch_shapes=[pltpu.VMEM((HI * PITCH, 128), F32)] * 2,
            input_output_aliases={3 + i: i for i in range(len(made))},
            cost_estimate=pl.CostEstimate(
                flops=40_000_000_000 // PARTS,
                bytes_accessed=n * HI * LO * 4 // PARTS,
                transcendentals=0,
            ),
        )
        made = call(hi, lo, v, *made)
    return made


def place(i):
    return {
        "x": i // 16 % 4,
        "y": i // 2 % 4,
        "z": i // 64 * 2 + i % 2,
        "core": i // 8 % 2,
    }


def device(at):
    return (((at["z"] // 2 * 4 + at["x"]) * 2 + at["core"]) * 4 + at["y"]) * 2 + at["z"] % 2


def shifted(value, dims, shift):
    pairs = []
    for i in range(128):
        at = place(i)
        dim = dims[at["core"]]
        at[dim] = (at[dim] + shift) % (2 if dim == "core" else 4)
        pairs.append((i, device(at)))
    return lax.ppermute(value, AXES, pairs)


def across(value):
    return shifted(value, ("core", "core"), 1)


def ring(value, dims):
    came = [value]
    for shift in SHIFTS:
        came.append(shifted(value, dims, shift))
    return jnp.concatenate(came, 0)


def summed_over_cols(value):
    for dim, bit in (("z", 1), ("y", 1), ("y", 2)):
        pairs = []
        for j in range(128):
            at = place(j)
            at[dim] ^= bit
            pairs.append((j, device(at)))
        other = lax.ppermute(value, AXES, pairs)
        value = value + other
    return value


def gather_tables(piece, second, core):
    half = piece.shape[1] // 2
    mine = lax.dynamic_slice_in_dim(piece, core * half, half, 1)
    other = lax.dynamic_slice_in_dim(piece, (1 - core) * half, half, 1)
    came = across(jnp.stack([other, second]))
    here = jnp.stack([mine, second])
    both = jnp.where(core == 0, jnp.stack([here, came]), jnp.stack([came, here]))
    unit = both[:, 0]
    close = ring(both[:, 1][None], ("x", "x"))
    remote = shifted(close, ("z", "z"), 2)
    near = ring(unit[None], ("x", "y"))
    plane = ring(near[None], ("y", "z"))
    last = ("z", "x")
    left = shifted(plane, last, 1)
    right = shifted(plane, last, -1)
    far0 = shifted(left[:2], last, 1)
    far1 = shifted(right[2:], last, -1)
    own = [x.reshape(-1, *unit.shape) for x in (plane, left, right, far0, far1)]
    return own, [across(x) for x in own], close, remote


def spot(there, here):
    ahead = (there - here) & 3
    return jnp.where(ahead == 3, 1, jnp.where(ahead == 0, 0, ahead + 1))


def pick_kernel(table, close_ref, remote_ref, index_ref, picked_ref, gram_ref, rows):
    half = rows.shape[0] // 2
    z_hi = table[4]
    near = jnp.concatenate([close_ref[table[x]].reshape(32, -1) for x in range(4)], 0)
    far = jnp.concatenate([remote_ref[table[x]].reshape(32, -1) for x in range(4)], 0)
    rows[pl.ds(pl.multiple_of(z_hi * half, half), half), :] = near
    rows[pl.ds(pl.multiple_of((1 - z_hi) * half, half), half), :] = far
    r = rows[...]
    gram_ref[...] = dot(r, r, NT)
    at = lax.broadcasted_iota(jnp.int32, (r.shape[1], index_ref.shape[1]), 0)
    hot = (at == index_ref[...]).astype(F32).astype(BF)
    picked_ref[...] = dot(r, hot, NN).T.astype(BF)


def pick(table, close, remote, index):
    n, rows = index.shape[1], close.shape[-1]
    return pl.pallas_call(
        pick_kernel,
        in_specs=[pl.BlockSpec(memory_space=pltpu.SMEM)]
        + [pl.BlockSpec(memory_space=pltpu.VMEM)] * 3,
        out_specs=[pl.BlockSpec(memory_space=pltpu.VMEM)] * 2,
        out_shape=[jax.ShapeDtypeStruct((n, 256), BF), jax.ShapeDtypeStruct((256, 256), F32)],
        scratch_shapes=[pltpu.VMEM((256, rows), BF)],
        cost_estimate=pl.CostEstimate(
            flops=2_000_000_000, bytes_accessed=2_000_000, transcendentals=0
        ),
    )(table, close, remote, index)


def piece_table(row_at, col_at, order):
    y, z_lo, z_hi, x = jnp.meshgrid(
        jnp.arange(4), jnp.arange(2), jnp.arange(2), jnp.arange(4), indexing="ij"
    )
    at_x = spot(x, row_at >> 1)
    at_y = spot(y, col_at >> 1)
    at_z = spot(z_hi * 2 + z_lo, (row_at >> 3) * 2 + (col_at & 1))
    first = jnp.where(order == 0, at_x, at_y)
    second = jnp.where(order == 0, at_y, at_z)
    third = jnp.where(order == 0, at_z, at_x)
    late = (third == 3) & (second >= 2)
    array = third + late
    index = (second - 2 * late) * 4 + first
    return jnp.concatenate([array.ravel(), index.ravel(), order[None]]).astype(jnp.int32)


def fetch(table, pieces, buf, sem, step, slot):
    n = buf.shape[1]
    for p in range(n):
        array = table[step * n + p]
        index = table[64 + step * n + p]
        for a, ref in enumerate(pieces):

            @pl.when(array == a)
            def _(ref=ref, p=p):
                pltpu.make_async_copy(ref.at[index], buf.at[slot, p], sem.at[slot]).start()


def accumulate(table, head_ref, rest_ref, pieces, fold_ref, gram_ref, buf, sem, begin):
    step = pl.program_id(0)
    slot = lax.rem(step, 2)

    @pl.when(step == 0)
    def _():
        begin()
        fetch(table, pieces, buf, sem, 0, 0)

    @pl.when(step + 1 < pl.num_programs(0))
    def _():
        fetch(table, pieces, buf, sem, step + 1, 1 - slot)

    pltpu.make_async_copy(pieces[0].at[pl.ds(0, buf.shape[1])], buf.at[slot], sem.at[slot]).wait()
    t = buf[slot].reshape(256, STEP * LO)
    head = jnp.concatenate([head_ref[i] for i in range(STEP)], 1)
    rest = jnp.concatenate([rest_ref[i] for i in range(STEP)], 1)
    fold_ref[...] += dot(head, t, NT) + dot(rest, t, NT)
    gram_ref[...] += dot(t, t, NT)


def first_kernel(table, head_ref, rest_ref, p0, p1, p2, p3, p4, fold_ref, gram_ref, buf, sem):
    def begin():
        fold_ref[...] = jnp.zeros_like(fold_ref)
        gram_ref[...] = jnp.zeros_like(gram_ref)

    accumulate(
        table, head_ref, rest_ref, (p0, p1, p2, p3, p4), fold_ref, gram_ref, buf, sem, begin
    )


def second_kernel(
    table, head_ref, rest_ref, p0, p1, p2, p3, p4,
    fold_in, gram_in, second_ref, owner_ref, part_ref, gram_ref, acc, buf, sem,
):
    def begin():
        acc[...] = fold_in[...]
        gram_ref[...] = gram_in[...]

    accumulate(table, head_ref, rest_ref, (p0, p1, p2, p3, p4), acc, gram_ref, buf, sem, begin)

    @pl.when(pl.program_id(0) == pl.num_programs(0) - 1)
    def _():
        head, rest = halves(second_ref[...].astype(F32) * acc[...])
        n = owner_ref.shape[1]
        slot = lax.broadcasted_iota(jnp.int32, (part_ref.shape[0], n), 0)
        hot = (slot == owner_ref[...]).astype(F32).astype(BF)
        part_ref[...] = dot(hot, head, NN) + dot(hot, rest, NN)


def product(table, head, rest, pieces, more, slab):
    n = head.shape[1]
    steps = HI // STEP // 2
    s_spec = pl.BlockSpec((STEP, n, LO), lambda i, table: (2 * i + table[128], 0, 0))
    any_spec = pl.BlockSpec(memory_space=pl.ANY)
    whole = lambda x: pl.BlockSpec(x.shape, lambda i, table: (0, 0))
    rows = slab if more else n
    out = [jax.ShapeDtypeStruct((rows, 256), F32), jax.ShapeDtypeStruct((256, 256), F32)]
    shape = pieces[0].shape
    scratch = [
        pltpu.VMEM((2, 8, *shape[1:]), BF),
        pltpu.SemaphoreType.DMA((2,)),
    ]
    if more:
        scratch = [pltpu.VMEM((n, 256), F32)] + scratch
    return pl.pallas_call(
        second_kernel if more else first_kernel,
        grid_spec=pltpu.PrefetchScalarGridSpec(
            num_scalar_prefetch=1,
            grid=(steps,),
            in_specs=[s_spec, s_spec] + [any_spec] * 5 + [whole(x) for x in more],
            out_specs=[whole(x) for x in out],
            scratch_shapes=scratch,
        ),
        out_shape=out,
        cost_estimate=pl.CostEstimate(
            flops=15_000_000_000, bytes_accessed=50_000_000, transcendentals=0
        ),
    )(table, head, rest, *pieces, *more)


def exact(a, b, dims):
    return lax.dot_general(a, b, dims, precision=lax.Precision.HIGHEST, preferred_element_type=F32)


def inverse_kernel(gram_ref, out_ref, ok_ref, a_ref, x_ref, r_ref):
    n = gram_ref.shape[0]
    at_row = lax.broadcasted_iota(jnp.int32, (n, n), 0)
    at_col = lax.broadcasted_iota(jnp.int32, (n, n), 1)
    eye = jnp.where(at_row == at_col, 1.0, 0.0)
    gram = gram_ref[...]
    diagonal = gram * eye
    by_row = lax.rsqrt(jnp.sum(diagonal, 1, keepdims=True))
    by_col = lax.rsqrt(jnp.sum(diagonal, 0, keepdims=True))
    a = gram * by_row * by_col
    bound = jnp.max(jnp.sum(jnp.abs(a), 0, keepdims=True))
    start = jnp.where(bound < 1.9, 1.0, 1.0 / bound)
    a_ref[...] = a
    x_ref[...] = start * eye
    r_ref[...] = eye - start * a

    def size(r):
        return jnp.sqrt(jnp.sum(r * r))

    def unfinished(state):
        i, now, before = state
        stuck = (now < 0.3) & (now > 0.5 * before)
        return (now > TOLERANCE) & (i < 40) & jnp.logical_not(stuck)

    def improve(state):
        i, now, _ = state
        x = x_ref[...] + exact(x_ref[...], r_ref[...], NN)
        r = eye - exact(a_ref[...], x, NN)
        x_ref[...] = x
        r_ref[...] = r
        return i + 1, size(r), now

    last = lax.while_loop(unfinished, improve, (0, size(r_ref[...]), jnp.float32(1e30)))
    x = x_ref[...] + exact(x_ref[...], r_ref[...], NN)
    out_ref[...] = x * by_row * by_col
    ok_ref[0] = jnp.where(last[1] <= TOLERANCE, 1, 0)


def inverse(gram):
    n = gram.shape[0]
    made, ok = pl.pallas_call(
        inverse_kernel,
        out_shape=[jax.ShapeDtypeStruct((n, n), F32), jax.ShapeDtypeStruct((1,), jnp.int32)],
        out_specs=[
            pl.BlockSpec(memory_space=pltpu.VMEM),
            pl.BlockSpec(memory_space=pltpu.SMEM),
        ],
        scratch_shapes=[pltpu.VMEM((n, n), F32)] * 3,
        cost_estimate=pl.CostEstimate(
            flops=5_000_000_000, bytes_accessed=600_000, transcendentals=0
        ),
    )(gram)

    def by_factor():
        factor = jnp.linalg.cholesky(gram)
        return jax.scipy.linalg.cho_solve((factor, True), jnp.eye(n, dtype=F32))

    return lax.cond(ok[0] == 1, lambda: made, by_factor)


def solve_kernel(inverse_ref, spread_ref, out_ref):
    total = spread_ref[0]
    for i in range(1, spread_ref.shape[0]):
        total = total + spread_ref[i]
    out_ref[...] = exact(inverse_ref[...], total, NT).reshape(out_ref.shape)


def solve(inverted, spread):
    n, rows = inverted.shape[0], spread.shape[1]
    return pl.pallas_call(
        solve_kernel,
        out_shape=jax.ShapeDtypeStruct((n // 16, 16, rows), F32),
        cost_estimate=pl.CostEstimate(
            flops=500_000_000, bytes_accessed=1_500_000, transcendentals=0
        ),
    )(inverted, spread)


def per_device(
    block_values,
    block_length,
    block_owner,
    block_second,
    block_third,
    live_blocks,
    second_factor,
    third_factor,
):
    n_rows = lax.axis_size("rows")
    n_cols = lax.axis_size("cols")
    row_at = lax.axis_index("rows")
    col_at = lax.axis_index("cols")
    nblk, width = block_values.shape
    range_rows = second_factor.shape[0]
    slab = range_rows * n_cols // n_rows

    core = row_at & 1
    own, swapped, close, remote = gather_tables(third_factor.T, second_factor.T, core)
    spots = jnp.concatenate(
        [spot(jnp.arange(4, dtype=jnp.int32), row_at >> 1), (row_at >> 3)[None]]
    )
    picked, local_gram = pick(
        spots, close, remote, (block_second - col_at * range_rows)[None, :]
    )
    gram_second = summed_over_cols(local_gram)

    lane = jnp.arange(width, dtype=jnp.int32)
    slot = jnp.arange(nblk, dtype=jnp.int32)
    live = (lane[None, :] < block_length[:, None]) & (slot < live_blocks[0])[:, None]
    values = jnp.where(live, block_values, jnp.zeros((), BF)).astype(F32)
    head, rest = build(
        (block_third // LO).astype(F32), (block_third % LO).astype(F32), values
    )
    owner = (block_owner - row_at * slab)[None, :]
    fold = product(piece_table(row_at, col_at, core), head, rest, own, (), slab)
    part, gram_third = product(
        piece_table(row_at, col_at, 1 - core), head, rest, swapped, (*fold, picked, owner), slab
    )

    gram = (gram_second / (range_rows * n_cols)) * (
        gram_third / (third_factor.shape[0] * n_cols)
    )
    spread = part.reshape(n_cols, slab // n_cols, -1)
    spread = lax.all_to_all(spread, "cols", 0, 0, tiled=True)
    solved = solve(inverse(gram), spread)
    moved = lax.all_to_all(solved, "rows", 0, 0, tiled=True)
    share = n_rows // n_cols
    moved = moved.reshape(n_cols, share, *solved.shape[1:])
    moved = lax.all_to_all(moved, "cols", 0, 0, tiled=True)
    return moved.transpose(1, 0, 3, 2).reshape(range_rows, solved.shape[1])


def solution(mesh):
    return jax.shard_map(
        per_device,
        mesh=mesh,
        in_specs=(
            P(("rows", "cols"), None),
            P(("rows", "cols")),
            P(("rows", "cols")),
            P(("rows", "cols")),
            P(("rows", "cols"), None),
            P(("rows", "cols")),
            P("cols", "rows"),
            P("cols", "rows"),
        ),
        out_specs=P("cols", "rows"),
        check_vma=False,
    )
```

```python
import functools

import jax
import jax.numpy as jnp
from jax import lax
from jax.experimental import pallas as pl
from jax.experimental.pallas import tpu as pltpu
from jax.sharding import PartitionSpec as P


BF = jnp.bfloat16
F32 = jnp.float32
NT = (((1,), (1,)), ((), ()))
NN = (((1,), (0,)), ((), ()))

LO = 256
HI = 128
NB = 16
PITCH = 140
GROUP = 64
PARTS = 4
STEP = 8
TOLERANCE = 3e-4
AXES = ("rows", "cols")
SHIFTS = (1, -1, 2)


def dot(a, b, dims):
    return lax.dot_general(a, b, dims, preferred_element_type=F32)


def halves(x):
    head = x.astype(BF)
    return head, (x - head.astype(F32)).astype(BF)


def prepare_kernel(
    live_ref, third_ref, value_ref, length_ref, hi_ref, lo_ref, v_ref, list_ref, count_ref, again
):
    step = pl.program_id(0)
    n, width = third_ref.shape
    third = third_ref[...]
    lane = lax.broadcasted_iota(jnp.int32, (n, width), 1)
    block = lax.broadcasted_iota(jnp.int32, (n, width), 0) + step * n
    live = (lane < length_ref[...]) & (block < live_ref[0])
    hi_ref[...] = (third >> 8).astype(F32)
    lo_ref[...] = (third & (LO - 1)).astype(F32)
    v_ref[...] = jnp.where(live, value_ref[...].astype(F32), 0.0)
    marked = jnp.where(live, third, -1 - lane)
    same = jnp.zeros((n, width), jnp.bool_)
    for shift in range(1, width // 2 + 1):
        same = same | (marked == pltpu.roll(marked, shift, 1))
    found = jnp.max(jnp.where(same, 1.0, 0.0), 1, keepdims=True)
    again[pl.ds(pl.multiple_of(step * n, n), n), :] = jnp.broadcast_to(found, (n, width))

    @pl.when(step == pl.num_programs(0) - 1)
    def _():
        total = again.shape[0]
        flags = again[...]
        row = lax.broadcasted_iota(jnp.int32, (total, total), 0)
        col = lax.broadcasted_iota(jnp.int32, (total, total), 1)
        earlier = jnp.where(col < row, 1.0, 0.0).astype(BF)
        ahead = dot(earlier, flags.astype(BF), NN)
        wide = jnp.concatenate([ahead] * (total // width), 1)
        on = jnp.concatenate([flags] * (total // width), 1)
        mine = (on > 0.5) & (wide == col.astype(F32))
        picked = jnp.sum(jnp.where(mine, row.astype(F32), 0.0), 0, keepdims=True)
        list_ref[...] = picked.astype(jnp.int32)
        count_ref[0] = jnp.sum(flags[:, :1]).astype(jnp.int32)


def prepare(third, values, length, live):
    n, width = third.shape
    rows = 128
    spec = pl.BlockSpec((rows, width), lambda i: (i, 0))
    shape = jax.ShapeDtypeStruct((n, width), F32)
    return pl.pallas_call(
        prepare_kernel,
        grid=(n // rows,),
        in_specs=[
            pl.BlockSpec(memory_space=pltpu.SMEM),
            spec,
            spec,
            pl.BlockSpec((rows, 1), lambda i: (i, 0)),
        ],
        out_specs=[spec] * 3
        + [pl.BlockSpec((1, n), lambda i: (0, 0)), pl.BlockSpec(memory_space=pltpu.SMEM)],
        out_shape=[shape] * 3
        + [jax.ShapeDtypeStruct((1, n), jnp.int32), jax.ShapeDtypeStruct((1,), jnp.int32)],
        scratch_shapes=[pltpu.VMEM((n, width), F32)],
        cost_estimate=pl.CostEstimate(
            flops=3_000_000_000, bytes_accessed=1_000_000, transcendentals=0
        ),
    )(live, third, values, length[:, None])


def spread_blocks(rows_of, left, right):
    base = lax.broadcasted_iota(jnp.int32, (16, 128), 0)
    iota = [(base + 16 * j).astype(F32).astype(BF) for j in range(LO // 16)]
    one = jnp.ones((16, 128), BF)
    zero = jnp.zeros((16, 128), BF)
    for b in range(NB):
        hi, lo, v = (jnp.broadcast_to(row, (16, 128)).astype(BF) for row in rows_of(b))
        a = jnp.concatenate([jnp.where(hi == iota[j], v, zero) for j in range(HI // 16)], 0)
        c = jnp.concatenate([jnp.where(lo == iota[j], one, zero) for j in range(LO // 16)], 0)
        s = dot(a, c, NT)
        left[b * PITCH : b * PITCH + HI, :] = s[:, :128]
        right[b * PITCH : b * PITCH + HI, :] = s[:, 128:]


def write_blocks(left, right, buf, out_ref, at, sem, value_of):
    quarter = HI // 4
    for q in range(4):

        def some(i, carry, q=q):
            for u in range(16):
                h = q * quarter + i * 16 + u
                blocks = pl.ds(h, NB, stride=PITCH)
                buf[h] = value_of(jnp.concatenate([left[blocks, :], right[blocks, :]], 1))
            return carry

        lax.fori_loop(0, quarter // 16, some, 0)
        rows = pl.ds(q * quarter, quarter)
        pltpu.make_async_copy(buf.at[rows], out_ref.at[rows, pl.ds(at, NB), :], sem).start()


def written(buf, out_ref, sem):
    return pltpu.make_async_copy(buf, out_ref.at[:, pl.ds(0, NB), :], sem)


def build_kernel(first, hi_ref, lo_ref, v_ref, *refs):
    head_ref, left, right, buf, sem = refs[-5:]
    step = pl.program_id(0)
    slot = lax.rem(step, 2)
    spread_blocks(
        lambda b: [ref[b : b + 1, :] for ref in (hi_ref, lo_ref, v_ref)], left, right
    )

    @pl.when(step >= 2)
    def _():
        written(buf.at[slot], head_ref, sem.at[slot]).wait()

    at = pl.multiple_of((first + step) * NB, NB)
    write_blocks(
        left, right, buf.at[slot], head_ref, at, sem.at[slot], lambda x: x.astype(BF)
    )

    @pl.when(step == pl.num_programs(0) - 1)
    def _():
        for i in range(2):
            written(buf.at[i], head_ref, sem.at[i]).wait()


def build(hi, lo, v):
    n = hi.shape[0]
    steps = n // NB // PARTS
    made = ()
    for part in range(PARTS):
        first = part * steps
        spec = pl.BlockSpec((NB, 128), lambda i, first=first: (first + i, 0))
        call = pl.pallas_call(
            functools.partial(build_kernel, first),
            grid=(steps,),
            in_specs=[spec] * 3 + [pl.BlockSpec(memory_space=pl.ANY)] * len(made),
            out_specs=pl.BlockSpec(memory_space=pl.ANY),
            out_shape=jax.ShapeDtypeStruct((HI, n, LO), BF),
            scratch_shapes=[pltpu.VMEM((NB * PITCH, 128), F32)] * 2
            + [pltpu.VMEM((2, HI, NB, LO), BF), pltpu.SemaphoreType.DMA((2,))],
            input_output_aliases={3: 0} if made else {},
            cost_estimate=pl.CostEstimate(
                flops=30_000_000_000 // PARTS,
                bytes_accessed=n * HI * LO * 2 // PARTS,
                transcendentals=0,
            ),
        )
        made = (call(hi, lo, v, *made),)
    return made[0]


def groups_of(count):
    return (count + GROUP - 1) // GROUP


def rest_kernel(count_ref, list_ref, hi_ref, lo_ref, v_ref, rest_ref, left, right, buf, sem):
    count = count_ref[0]

    def some(i, carry):
        def rows_of(b):
            slot = i * NB + b
            block = list_ref[0, slot]
            on = jnp.where(slot < count, 1.0, 0.0).astype(F32)
            hi, lo, v = (ref[pl.ds(block, 1), :] for ref in (hi_ref, lo_ref, v_ref))
            return hi, lo, v * on

        spread_blocks(rows_of, left, right)

        @pl.when(i > 0)
        def _():
            written(buf, rest_ref, sem).wait()

        at = pl.multiple_of(i * NB, NB)
        write_blocks(
            left, right, buf, rest_ref, at, sem, lambda x: (x - x.astype(BF).astype(F32)).astype(BF)
        )
        return carry

    lax.fori_loop(0, groups_of(count) * (GROUP // NB), some, 0)

    @pl.when(count > 0)
    def _():
        written(buf, rest_ref, sem).wait()


def build_rest(count, listed, hi, lo, v):
    n = hi.shape[0]
    return pl.pallas_call(
        rest_kernel,
        in_specs=[pl.BlockSpec(memory_space=pltpu.SMEM)] * 2
        + [pl.BlockSpec(memory_space=pltpu.VMEM)] * 3,
        out_specs=pl.BlockSpec(memory_space=pl.ANY),
        out_shape=jax.ShapeDtypeStruct((HI, n, LO), BF),
        scratch_shapes=[pltpu.VMEM((NB * PITCH, 128), F32)] * 2
        + [pltpu.VMEM((HI, NB, LO), BF), pltpu.SemaphoreType.DMA],
        cost_estimate=pl.CostEstimate(
            flops=6_000_000_000, bytes_accessed=6_000_000, transcendentals=0
        ),
    )(count, listed, hi, lo, v)


def place(i):
    return {
        "x": i // 16 % 4,
        "y": i // 2 % 4,
        "z": i // 64 * 2 + i % 2,
        "core": i // 8 % 2,
    }


def device(at):
    return (((at["z"] // 2 * 4 + at["x"]) * 2 + at["core"]) * 4 + at["y"]) * 2 + at["z"] % 2


def shifted(value, dims, shift):
    pairs = []
    for i in range(128):
        at = place(i)
        dim = dims[at["core"]]
        at[dim] = (at[dim] + shift) % (2 if dim == "core" else 4)
        pairs.append((i, device(at)))
    return lax.ppermute(value, AXES, pairs)


def across(value):
    return shifted(value, ("core", "core"), 1)


def ring(value, dims):
    came = [value]
    for shift in SHIFTS:
        came.append(shifted(value, dims, shift))
    return jnp.concatenate(came, 0)


def summed_over_cols(value):
    for dim, bit in (("z", 1), ("y", 1), ("y", 2)):
        pairs = []
        for j in range(128):
            at = place(j)
            at[dim] ^= bit
            pairs.append((j, device(at)))
        other = lax.ppermute(value, AXES, pairs)
        value = value + other
    return value


def gather_tables(piece, second, core):
    half = piece.shape[1] // 2
    mine = lax.dynamic_slice_in_dim(piece, core * half, half, 1)
    other = lax.dynamic_slice_in_dim(piece, (1 - core) * half, half, 1)
    came = across(jnp.stack([other, second]))
    here = jnp.stack([mine, second])
    both = jnp.where(core == 0, jnp.stack([here, came]), jnp.stack([came, here]))
    unit = both[:, 0]
    close = ring(both[:, 1][None], ("x", "x"))
    remote = shifted(close, ("z", "z"), 2)
    near = ring(unit[None], ("x", "y"))
    plane = ring(near[None], ("y", "z"))
    last = ("z", "x")
    left = shifted(plane, last, 1)
    right = shifted(plane, last, -1)
    far0 = shifted(left[:2], last, 1)
    far1 = shifted(right[2:], last, -1)
    own = [x.reshape(-1, *unit.shape) for x in (plane, left, right, far0, far1)]
    return own, [across(x) for x in own], close, remote


def spot(there, here):
    ahead = (there - here) & 3
    return jnp.where(ahead == 3, 1, jnp.where(ahead == 0, 0, ahead + 1))


def pick_kernel(table, close_ref, remote_ref, index_ref, picked_ref, gram_ref, rows):
    half = rows.shape[0] // 2
    z_hi = table[4]
    near = jnp.concatenate([close_ref[table[x]].reshape(32, -1) for x in range(4)], 0)
    far = jnp.concatenate([remote_ref[table[x]].reshape(32, -1) for x in range(4)], 0)
    rows[pl.ds(pl.multiple_of(z_hi * half, half), half), :] = near
    rows[pl.ds(pl.multiple_of((1 - z_hi) * half, half), half), :] = far
    r = rows[...]
    gram_ref[...] = dot(r, r, NT)
    at = lax.broadcasted_iota(jnp.int32, (r.shape[1], index_ref.shape[1]), 0)
    hot = (at == index_ref[...]).astype(F32).astype(BF)
    picked_ref[...] = dot(r, hot, NN).T.astype(BF)


def pick(table, close, remote, index):
    n, rows = index.shape[1], close.shape[-1]
    return pl.pallas_call(
        pick_kernel,
        in_specs=[pl.BlockSpec(memory_space=pltpu.SMEM)]
        + [pl.BlockSpec(memory_space=pltpu.VMEM)] * 3,
        out_specs=[pl.BlockSpec(memory_space=pltpu.VMEM)] * 2,
        out_shape=[jax.ShapeDtypeStruct((n, 256), BF), jax.ShapeDtypeStruct((256, 256), F32)],
        scratch_shapes=[pltpu.VMEM((256, rows), BF)],
        cost_estimate=pl.CostEstimate(
            flops=2_000_000_000, bytes_accessed=2_000_000, transcendentals=0
        ),
    )(table, close, remote, index)


def piece_table(row_at, col_at, order):
    y, z_lo, z_hi, x = jnp.meshgrid(
        jnp.arange(4), jnp.arange(2), jnp.arange(2), jnp.arange(4), indexing="ij"
    )
    at_x = spot(x, row_at >> 1)
    at_y = spot(y, col_at >> 1)
    at_z = spot(z_hi * 2 + z_lo, (row_at >> 3) * 2 + (col_at & 1))
    first = jnp.where(order == 0, at_x, at_y)
    second = jnp.where(order == 0, at_y, at_z)
    third = jnp.where(order == 0, at_z, at_x)
    late = (third == 3) & (second >= 2)
    array = third + late
    index = (second - 2 * late) * 4 + first
    return jnp.concatenate([array.ravel(), index.ravel(), order[None]]).astype(jnp.int32)


def fetch(table, count, rest, pieces, buf, rest_buf, sem, rest_sem, step, slot):
    n = buf.shape[1]
    for p in range(n):
        array = table[step * n + p]
        index = table[64 + step * n + p]
        for a, ref in enumerate(pieces):

            @pl.when(array == a)
            def _(ref=ref, p=p):
                pltpu.make_async_copy(ref.at[index], buf.at[slot, p], sem.at[slot]).start()

    @pl.when(count > 0)
    def _():
        rest_copy(table, rest, rest_buf, rest_sem, step, slot, 0).start()


def rest_copy(table, rest, rest_buf, rest_sem, step, slot, group):
    first = pl.multiple_of((2 * step + table[128]) * STEP, STEP)
    at = pl.multiple_of(group * GROUP, GROUP)
    return pltpu.make_async_copy(
        rest.at[pl.ds(first, STEP), pl.ds(at, GROUP), :], rest_buf.at[slot], rest_sem.at[slot]
    )


def accumulate(table, count_ref, head_ref, rest, pieces, sums, bufs, begin):
    fold_ref, gram_ref, extra_ref = sums
    buf, rest_buf, sem, rest_sem = bufs
    step = pl.program_id(0)
    slot = lax.rem(step, 2)
    count = count_ref[0]

    @pl.when(step == 0)
    def _():
        begin()
        fetch(table, count, rest, pieces, *bufs, 0, 0)

        @pl.when(count == 0)
        def _():
            rest_buf[...] = jnp.zeros_like(rest_buf)

    @pl.when(step + 1 < pl.num_programs(0))
    def _():
        fetch(table, count, rest, pieces, *bufs, step + 1, 1 - slot)

    pltpu.make_async_copy(pieces[0].at[pl.ds(0, buf.shape[1])], buf.at[slot], sem.at[slot]).wait()

    @pl.when(count > 0)
    def _():
        rest_copy(table, rest, rest_buf, rest_sem, step, slot, 0).wait()

    def listed(at):
        return jnp.concatenate([rest_buf[at, i] for i in range(STEP)], 1)

    t = buf[slot].reshape(256, STEP * LO)
    head = jnp.concatenate([head_ref[i] for i in range(STEP)], 1)
    fold_ref[...] += dot(head, t, NT)
    both = dot(jnp.concatenate([t, listed(slot)], 0), t, NT)
    gram_ref[...] += both[:256]
    extra_ref[:GROUP] += both[256:]

    def more(group, carry):
        copy = rest_copy(table, rest, rest_buf, rest_sem, step, slot, group)
        copy.start()
        copy.wait()
        at = pl.multiple_of(group * GROUP, GROUP)
        extra_ref[pl.ds(at, GROUP), :] += dot(listed(slot), buf[slot].reshape(256, STEP * LO), NT)
        return carry

    lax.fori_loop(1, groups_of(count), more, 0)


def first_kernel(
    table, count_ref, head_ref, rest, p0, p1, p2, p3, p4, fold_ref, gram_ref, extra_ref, *bufs
):
    sums = (fold_ref, gram_ref, extra_ref)

    def begin():
        for ref in sums:
            ref[...] = jnp.zeros_like(ref)

    accumulate(table, count_ref, head_ref, rest, (p0, p1, p2, p3, p4), sums, bufs, begin)


def second_kernel(
    table, count_ref, head_ref, rest, p0, p1, p2, p3, p4, fold_in, gram_in, extra_in,
    second_ref, owner_ref, list_ref, part_ref, gram_ref, fold_ref, extra_ref, *bufs,
):
    def begin():
        fold_ref[...] = fold_in[...]
        gram_ref[...] = gram_in[...]
        extra_ref[...] = extra_in[...]

    sums = (fold_ref, gram_ref, extra_ref)
    accumulate(table, count_ref, head_ref, rest, (p0, p1, p2, p3, p4), sums, bufs, begin)

    @pl.when(pl.program_id(0) == pl.num_programs(0) - 1)
    def _():
        n = owner_ref.shape[1]
        block = lax.broadcasted_iota(jnp.int32, (n, n), 0)
        place = lax.broadcasted_iota(jnp.int32, (n, n), 1)
        own = (block == list_ref[...]) & (place < count_ref[0])
        own = jnp.where(own, 1.0, 0.0).astype(BF)
        head, rest = halves(extra_ref[...])
        fold = fold_ref[...] + (dot(own, head, NN) + dot(own, rest, NN))
        head, rest = halves(second_ref[...].astype(F32) * fold)
        slot = lax.broadcasted_iota(jnp.int32, (part_ref.shape[0], n), 0)
        hot = (slot == owner_ref[...]).astype(F32).astype(BF)
        part_ref[...] = dot(hot, head, NN) + dot(hot, rest, NN)


def product(table, count, head, rest, pieces, more, slab):
    n = head.shape[1]
    steps = HI // STEP // 2
    any_spec = pl.BlockSpec(memory_space=pl.ANY)
    whole = lambda x: pl.BlockSpec(x.shape, lambda i, *scalars: (0, 0))
    sums = [jax.ShapeDtypeStruct((rows, 256), F32) for rows in (n, 256, n)]
    out = [jax.ShapeDtypeStruct((slab, 256), F32), sums[1]] if more else sums
    scratch = [
        pltpu.VMEM((2, 8, *pieces[0].shape[1:]), BF),
        pltpu.VMEM((2, STEP, GROUP, LO), BF),
        pltpu.SemaphoreType.DMA((2,)),
        pltpu.SemaphoreType.DMA((2,)),
    ]
    if more:
        scratch = [pltpu.VMEM((n, 256), F32)] * 2 + scratch
    return pl.pallas_call(
        second_kernel if more else first_kernel,
        grid_spec=pltpu.PrefetchScalarGridSpec(
            num_scalar_prefetch=2,
            grid=(steps,),
            in_specs=[
                pl.BlockSpec((STEP, n, LO), lambda i, table, count: (2 * i + table[128], 0, 0))
            ]
            + [any_spec] * 6
            + [whole(x) for x in more],
            out_specs=[whole(x) for x in out],
            scratch_shapes=scratch,
        ),
        out_shape=out,
        cost_estimate=pl.CostEstimate(
            flops=15_000_000_000, bytes_accessed=30_000_000, transcendentals=0
        ),
    )(table, count, head, rest, *pieces, *more)


def exact(a, b, dims):
    return lax.dot_general(a, b, dims, precision=lax.Precision.HIGHEST, preferred_element_type=F32)


def inverse_kernel(gram_ref, out_ref, ok_ref, a_ref, x_ref, r_ref):
    n = gram_ref.shape[0]
    at_row = lax.broadcasted_iota(jnp.int32, (n, n), 0)
    at_col = lax.broadcasted_iota(jnp.int32, (n, n), 1)
    eye = jnp.where(at_row == at_col, 1.0, 0.0)
    gram = gram_ref[...]
    diagonal = gram * eye
    by_row = lax.rsqrt(jnp.sum(diagonal, 1, keepdims=True))
    by_col = lax.rsqrt(jnp.sum(diagonal, 0, keepdims=True))
    a = gram * by_row * by_col
    bound = jnp.max(jnp.sum(jnp.abs(a), 0, keepdims=True))
    start = jnp.where(bound < 1.9, 1.0, 1.0 / bound)
    a_ref[...] = a
    x_ref[...] = start * eye
    r_ref[...] = eye - start * a

    def size(r):
        return jnp.sqrt(jnp.sum(r * r))

    def unfinished(state):
        i, now, before = state
        stuck = (now < 0.3) & (now > 0.5 * before)
        return (now > TOLERANCE) & (i < 40) & jnp.logical_not(stuck)

    def improve(state):
        i, now, _ = state
        x = x_ref[...] + exact(x_ref[...], r_ref[...], NN)
        r = eye - exact(a_ref[...], x, NN)
        x_ref[...] = x
        r_ref[...] = r
        return i + 1, size(r), now

    last = lax.while_loop(unfinished, improve, (0, size(r_ref[...]), jnp.float32(1e30)))
    x = x_ref[...] + exact(x_ref[...], r_ref[...], NN)
    out_ref[...] = x * by_row * by_col
    ok_ref[0] = jnp.where(last[1] <= TOLERANCE, 1, 0)


def inverse(gram):
    n = gram.shape[0]
    made, ok = pl.pallas_call(
        inverse_kernel,
        out_shape=[jax.ShapeDtypeStruct((n, n), F32), jax.ShapeDtypeStruct((1,), jnp.int32)],
        out_specs=[
            pl.BlockSpec(memory_space=pltpu.VMEM),
            pl.BlockSpec(memory_space=pltpu.SMEM),
        ],
        scratch_shapes=[pltpu.VMEM((n, n), F32)] * 3,
        cost_estimate=pl.CostEstimate(
            flops=5_000_000_000, bytes_accessed=600_000, transcendentals=0
        ),
    )(gram)

    def by_factor():
        factor = jnp.linalg.cholesky(gram)
        return jax.scipy.linalg.cho_solve((factor, True), jnp.eye(n, dtype=F32))

    return lax.cond(ok[0] == 1, lambda: made, by_factor)


def solve_kernel(inverse_ref, spread_ref, out_ref):
    total = spread_ref[0]
    for i in range(1, spread_ref.shape[0]):
        total = total + spread_ref[i]
    out_ref[...] = exact(inverse_ref[...], total, NT).reshape(out_ref.shape)


def solve(inverted, spread):
    n, rows = inverted.shape[0], spread.shape[1]
    return pl.pallas_call(
        solve_kernel,
        out_shape=jax.ShapeDtypeStruct((n // 16, 16, rows), F32),
        cost_estimate=pl.CostEstimate(
            flops=500_000_000, bytes_accessed=1_500_000, transcendentals=0
        ),
    )(inverted, spread)


def per_device(
    block_values,
    block_length,
    block_owner,
    block_second,
    block_third,
    live_blocks,
    second_factor,
    third_factor,
):
    n_rows = lax.axis_size("rows")
    n_cols = lax.axis_size("cols")
    row_at = lax.axis_index("rows")
    col_at = lax.axis_index("cols")
    range_rows = second_factor.shape[0]
    slab = range_rows * n_cols // n_rows

    core = row_at & 1
    own, swapped, close, remote = gather_tables(third_factor.T, second_factor.T, core)
    spots = jnp.concatenate(
        [spot(jnp.arange(4, dtype=jnp.int32), row_at >> 1), (row_at >> 3)[None]]
    )
    picked, local_gram = pick(
        spots, close, remote, (block_second - col_at * range_rows)[None, :]
    )
    gram_second = summed_over_cols(local_gram)

    hi, lo, v, listed, count = prepare(block_third, block_values, block_length, live_blocks)
    head = build(hi, lo, v)
    rest = build_rest(count, listed, hi, lo, v)
    owner = (block_owner - row_at * slab)[None, :]
    sums = product(piece_table(row_at, col_at, core), count, head, rest, own, (), slab)
    part, gram_third = product(
        piece_table(row_at, col_at, 1 - core),
        count,
        head,
        rest,
        swapped,
        (*sums, picked, owner, listed),
        slab,
    )

    gram = (gram_second / (range_rows * n_cols)) * (
        gram_third / (third_factor.shape[0] * n_cols)
    )
    spread = part.reshape(n_cols, slab // n_cols, -1)
    spread = lax.all_to_all(spread, "cols", 0, 0, tiled=True)
    solved = solve(inverse(gram), spread)
    moved = lax.all_to_all(solved, "rows", 0, 0, tiled=True)
    share = n_rows // n_cols
    moved = moved.reshape(n_cols, share, *solved.shape[1:])
    moved = lax.all_to_all(moved, "cols", 0, 0, tiled=True)
    return moved.transpose(1, 0, 3, 2).reshape(range_rows, solved.shape[1])


def solution(mesh):
    return jax.shard_map(
        per_device,
        mesh=mesh,
        in_specs=(
            P(("rows", "cols"), None),
            P(("rows", "cols")),
            P(("rows", "cols")),
            P(("rows", "cols")),
            P(("rows", "cols"), None),
            P(("rows", "cols")),
            P("cols", "rows"),
            P("cols", "rows"),
        ),
        out_specs=P("cols", "rows"),
        check_vma=False,
    )
```

```python
import functools

import jax
import jax.numpy as jnp
from jax import lax
from jax.experimental import pallas as pl
from jax.experimental.pallas import tpu as pltpu
from jax.sharding import PartitionSpec as P


BF = jnp.bfloat16
F32 = jnp.float32
NT = (((1,), (1,)), ((), ()))
NN = (((1,), (0,)), ((), ()))

LO = 256
HI = 128
NB = 16
PITCH = 140
GROUP = 64
PARTS = 4
STEP = 8
TOLERANCE = 3e-4
AXES = ("rows", "cols")
SHIFTS = (1, -1, 2)


def dot(a, b, dims):
    return lax.dot_general(a, b, dims, preferred_element_type=F32)


def halves(x):
    head = x.astype(BF)
    return head, (x - head.astype(F32)).astype(BF)


def prepare_kernel(
    live_ref, third_ref, value_ref, length_ref, hi_ref, lo_ref, v_ref, list_ref, count_ref, again
):
    step = pl.program_id(0)
    n, width = third_ref.shape
    third = third_ref[...]
    lane = lax.broadcasted_iota(jnp.int32, (n, width), 1)
    block = lax.broadcasted_iota(jnp.int32, (n, width), 0) + step * n
    across = lax.broadcasted_iota(jnp.int32, (n, width), 0) == lane
    length = jnp.sum(jnp.where(across, length_ref[...].astype(F32), 0.0), 1, keepdims=True)
    live = (lane.astype(F32) < length) & (block < live_ref[0])
    hi_ref[...] = (third >> 8).astype(F32)
    lo_ref[...] = (third & (LO - 1)).astype(F32)
    v_ref[...] = jnp.where(live, value_ref[...].astype(F32), 0.0)
    marked = jnp.where(live, third, (1 << 15) + lane)
    pair = marked[: n // 2] | (marked[n // 2 :] << 16)
    low = jnp.zeros_like(pair)
    high = jnp.zeros_like(pair)
    for shift in range(1, width // 2 + 1):
        differ = pair ^ pltpu.roll(pair, shift, 1)
        low = low | ((differ & 0xFFFF) - 1)
        high = high | (lax.shift_right_logical(differ, 16) - 1)
    same = jnp.concatenate([jnp.where(x < 0, 1.0, 0.0) for x in (low, high)], 0)
    found = jnp.max(same, 1, keepdims=True)
    again[pl.ds(pl.multiple_of(step * n, n), n), :] = jnp.broadcast_to(found, (n, width))

    @pl.when(step == pl.num_programs(0) - 1)
    def _():
        total = again.shape[0]
        flags = again[...]
        row = lax.broadcasted_iota(jnp.int32, (total, total), 0)
        col = lax.broadcasted_iota(jnp.int32, (total, total), 1)
        earlier = jnp.where(col < row, 1.0, 0.0).astype(BF)
        ahead = dot(earlier, flags.astype(BF), NN)
        wide = jnp.concatenate([ahead] * (total // width), 1)
        on = jnp.concatenate([flags] * (total // width), 1)
        mine = (on > 0.5) & (wide == col.astype(F32))
        picked = jnp.sum(jnp.where(mine, row.astype(F32), 0.0), 0, keepdims=True)
        list_ref[...] = picked.astype(jnp.int32)
        count_ref[0] = jnp.sum(flags[:, :1]).astype(jnp.int32)


def prepare(third, values, length, live):
    n, width = third.shape
    rows = 128
    spec = pl.BlockSpec((rows, width), lambda i: (i, 0))
    shape = jax.ShapeDtypeStruct((n, width), F32)
    return pl.pallas_call(
        prepare_kernel,
        grid=(n // rows,),
        in_specs=[
            pl.BlockSpec(memory_space=pltpu.SMEM),
            spec,
            spec,
            pl.BlockSpec((1, rows), lambda i: (0, i)),
        ],
        out_specs=[spec] * 3
        + [pl.BlockSpec((1, n), lambda i: (0, 0)), pl.BlockSpec(memory_space=pltpu.SMEM)],
        out_shape=[shape] * 3
        + [jax.ShapeDtypeStruct((1, n), jnp.int32), jax.ShapeDtypeStruct((1,), jnp.int32)],
        scratch_shapes=[pltpu.VMEM((n, width), F32)],
        cost_estimate=pl.CostEstimate(
            flops=3_000_000_000, bytes_accessed=1_000_000, transcendentals=0
        ),
    )(live, third, values, length[None, :])


def spread_blocks(rows_of, left, right):
    base = lax.broadcasted_iota(jnp.int32, (16, 128), 0)
    iota = [(base + 16 * j).astype(F32).astype(BF) for j in range(LO // 16)]
    one = jnp.ones((16, 128), BF)
    zero = jnp.zeros((16, 128), BF)
    for b in range(NB):
        hi, lo, v = (jnp.broadcast_to(row, (16, 128)).astype(BF) for row in rows_of(b))
        a = jnp.concatenate([jnp.where(hi == iota[j], v, zero) for j in range(HI // 16)], 0)
        c = jnp.concatenate([jnp.where(lo == iota[j], one, zero) for j in range(LO // 16)], 0)
        s = dot(a, c, NT)
        left[b * PITCH : b * PITCH + HI, :] = s[:, :128]
        right[b * PITCH : b * PITCH + HI, :] = s[:, 128:]


def write_blocks(left, right, buf, out_ref, at, sem, value_of):
    quarter = HI // 4
    for q in range(4):

        def some(i, carry, q=q):
            for u in range(16):
                h = q * quarter + i * 16 + u
                blocks = pl.ds(h, NB, stride=PITCH)
                buf[h] = value_of(jnp.concatenate([left[blocks, :], right[blocks, :]], 1))
            return carry

        lax.fori_loop(0, quarter // 16, some, 0)
        rows = pl.ds(q * quarter, quarter)
        pltpu.make_async_copy(buf.at[rows], out_ref.at[rows, pl.ds(at, NB), :], sem).start()


def written(buf, out_ref, sem):
    return pltpu.make_async_copy(buf, out_ref.at[:, pl.ds(0, NB), :], sem)


def build_kernel(first, hi_ref, lo_ref, v_ref, *refs):
    head_ref, left, right, buf, sem = refs[-5:]
    step = pl.program_id(0)
    slot = lax.rem(step, 2)
    spread_blocks(
        lambda b: [ref[b : b + 1, :] for ref in (hi_ref, lo_ref, v_ref)], left, right
    )

    @pl.when(step >= 2)
    def _():
        written(buf.at[slot], head_ref, sem.at[slot]).wait()

    at = pl.multiple_of((first + step) * NB, NB)
    write_blocks(
        left, right, buf.at[slot], head_ref, at, sem.at[slot], lambda x: x.astype(BF)
    )

    @pl.when(step == pl.num_programs(0) - 1)
    def _():
        for i in range(2):
            written(buf.at[i], head_ref, sem.at[i]).wait()


def build(hi, lo, v):
    n = hi.shape[0]
    steps = n // NB // PARTS
    made = ()
    for part in range(PARTS):
        first = part * steps
        spec = pl.BlockSpec((NB, 128), lambda i, first=first: (first + i, 0))
        call = pl.pallas_call(
            functools.partial(build_kernel, first),
            grid=(steps,),
            in_specs=[spec] * 3 + [pl.BlockSpec(memory_space=pl.ANY)] * len(made),
            out_specs=pl.BlockSpec(memory_space=pl.ANY),
            out_shape=jax.ShapeDtypeStruct((HI, n, LO), BF),
            scratch_shapes=[pltpu.VMEM((NB * PITCH, 128), F32)] * 2
            + [pltpu.VMEM((2, HI, NB, LO), BF), pltpu.SemaphoreType.DMA((2,))],
            input_output_aliases={3: 0} if made else {},
            cost_estimate=pl.CostEstimate(
                flops=30_000_000_000 // PARTS,
                bytes_accessed=n * HI * LO * 2 // PARTS,
                transcendentals=0,
            ),
        )
        made = (call(hi, lo, v, *made),)
    return made[0]


def groups_of(count):
    return (count + GROUP - 1) // GROUP


def rest_kernel(count_ref, list_ref, hi_ref, lo_ref, v_ref, rest_ref, left, right, buf, sem):
    count = count_ref[0]

    def some(i, carry):
        def rows_of(b):
            slot = i * NB + b
            block = list_ref[0, slot]
            on = jnp.where(slot < count, 1.0, 0.0).astype(F32)
            hi, lo, v = (ref[pl.ds(block, 1), :] for ref in (hi_ref, lo_ref, v_ref))
            return hi, lo, v * on

        spread_blocks(rows_of, left, right)

        @pl.when(i > 0)
        def _():
            written(buf, rest_ref, sem).wait()

        at = pl.multiple_of(i * NB, NB)
        write_blocks(
            left, right, buf, rest_ref, at, sem, lambda x: (x - x.astype(BF).astype(F32)).astype(BF)
        )
        return carry

    lax.fori_loop(0, groups_of(count) * (GROUP // NB), some, 0)

    @pl.when(count > 0)
    def _():
        written(buf, rest_ref, sem).wait()


def build_rest(count, listed, hi, lo, v):
    n = hi.shape[0]
    return pl.pallas_call(
        rest_kernel,
        in_specs=[pl.BlockSpec(memory_space=pltpu.SMEM)] * 2
        + [pl.BlockSpec(memory_space=pltpu.VMEM)] * 3,
        out_specs=pl.BlockSpec(memory_space=pl.ANY),
        out_shape=jax.ShapeDtypeStruct((HI, n, LO), BF),
        scratch_shapes=[pltpu.VMEM((NB * PITCH, 128), F32)] * 2
        + [pltpu.VMEM((HI, NB, LO), BF), pltpu.SemaphoreType.DMA],
        cost_estimate=pl.CostEstimate(
            flops=6_000_000_000, bytes_accessed=6_000_000, transcendentals=0
        ),
    )(count, listed, hi, lo, v)


def place(i):
    return {
        "x": i // 16 % 4,
        "y": i // 2 % 4,
        "z": i // 64 * 2 + i % 2,
        "core": i // 8 % 2,
    }


def device(at):
    return (((at["z"] // 2 * 4 + at["x"]) * 2 + at["core"]) * 4 + at["y"]) * 2 + at["z"] % 2


def shifted(value, dims, shift):
    pairs = []
    for i in range(128):
        at = place(i)
        dim = dims[at["core"]]
        at[dim] = (at[dim] + shift) % (2 if dim == "core" else 4)
        pairs.append((i, device(at)))
    return lax.ppermute(value, AXES, pairs)


def across(value):
    return shifted(value, ("core", "core"), 1)


def ring(value, dims):
    came = [value]
    for shift in SHIFTS:
        came.append(shifted(value, dims, shift))
    return jnp.concatenate(came, 0)


def summed_over_cols(value):
    for dim, bit in (("z", 1), ("y", 1), ("y", 2)):
        pairs = []
        for j in range(128):
            at = place(j)
            at[dim] ^= bit
            pairs.append((j, device(at)))
        other = lax.ppermute(value, AXES, pairs)
        value = value + other
    return value


def gather_tables(piece, second, core):
    half = piece.shape[1] // 2
    mine = lax.dynamic_slice_in_dim(piece, core * half, half, 1)
    other = lax.dynamic_slice_in_dim(piece, (1 - core) * half, half, 1)
    came = across(jnp.stack([other, second]))
    here = jnp.stack([mine, second])
    both = jnp.where(core == 0, jnp.stack([here, came]), jnp.stack([came, here]))
    unit = both[:, 0]
    close = ring(both[:, 1][None], ("x", "x"))
    remote = shifted(close, ("z", "z"), 2)
    near = ring(unit[None], ("x", "y"))
    plane = ring(near[None], ("y", "z"))
    last = ("z", "x")
    left = shifted(plane, last, 1)
    right = shifted(plane, last, -1)
    far0 = shifted(left[:2], last, 1)
    far1 = shifted(right[2:], last, -1)
    own = [x.reshape(-1, *unit.shape) for x in (plane, left, right, far0, far1)]
    return own, [across(x) for x in own], close, remote


def spot(there, here):
    ahead = (there - here) & 3
    return jnp.where(ahead == 3, 1, jnp.where(ahead == 0, 0, ahead + 1))


def pick_kernel(table, close_ref, remote_ref, index_ref, picked_ref, gram_ref, rows):
    half = rows.shape[0] // 2
    z_hi = table[4]
    near = jnp.concatenate([close_ref[table[x]].reshape(32, -1) for x in range(4)], 0)
    far = jnp.concatenate([remote_ref[table[x]].reshape(32, -1) for x in range(4)], 0)
    rows[pl.ds(pl.multiple_of(z_hi * half, half), half), :] = near
    rows[pl.ds(pl.multiple_of((1 - z_hi) * half, half), half), :] = far
    r = rows[...]
    gram_ref[...] = dot(r, r, NT)
    at = lax.broadcasted_iota(jnp.int32, (r.shape[1], index_ref.shape[1]), 0)
    hot = (at == index_ref[...] - table[5]).astype(F32).astype(BF)
    picked_ref[...] = dot(r, hot, NN).T.astype(BF)


def pick(table, close, remote, index):
    n, rows = index.shape[1], close.shape[-1]
    return pl.pallas_call(
        pick_kernel,
        in_specs=[pl.BlockSpec(memory_space=pltpu.SMEM)]
        + [pl.BlockSpec(memory_space=pltpu.VMEM)] * 3,
        out_specs=[pl.BlockSpec(memory_space=pltpu.VMEM)] * 2,
        out_shape=[jax.ShapeDtypeStruct((n, 256), BF), jax.ShapeDtypeStruct((256, 256), F32)],
        scratch_shapes=[pltpu.VMEM((256, rows), BF)],
        cost_estimate=pl.CostEstimate(
            flops=2_000_000_000, bytes_accessed=2_000_000, transcendentals=0
        ),
    )(table, close, remote, index)


def piece_table(row_at, col_at, order, slab):
    y, z_lo, z_hi, x = jnp.meshgrid(
        jnp.arange(4), jnp.arange(2), jnp.arange(2), jnp.arange(4), indexing="ij"
    )
    at_x = spot(x, row_at >> 1)
    at_y = spot(y, col_at >> 1)
    at_z = spot(z_hi * 2 + z_lo, (row_at >> 3) * 2 + (col_at & 1))
    first = jnp.where(order == 0, at_x, at_y)
    second = jnp.where(order == 0, at_y, at_z)
    third = jnp.where(order == 0, at_z, at_x)
    late = (third == 3) & (second >= 2)
    array = third + late
    index = (second - 2 * late) * 4 + first
    last = jnp.stack([order, row_at * slab])
    return jnp.concatenate([array.ravel(), index.ravel(), last]).astype(jnp.int32)


def fetch(table, count, rest, pieces, buf, rest_buf, sem, rest_sem, step, slot):
    n = buf.shape[1]
    for p in range(n):
        array = table[step * n + p]
        index = table[64 + step * n + p]
        for a, ref in enumerate(pieces):

            @pl.when(array == a)
            def _(ref=ref, p=p):
                pltpu.make_async_copy(ref.at[index], buf.at[slot, p], sem.at[slot]).start()

    @pl.when(count > 0)
    def _():
        rest_copy(table, rest, rest_buf, rest_sem, step, slot, 0).start()


def rest_copy(table, rest, rest_buf, rest_sem, step, slot, group):
    first = pl.multiple_of((2 * step + table[128]) * STEP, STEP)
    at = pl.multiple_of(group * GROUP, GROUP)
    return pltpu.make_async_copy(
        rest.at[pl.ds(first, STEP), pl.ds(at, GROUP), :], rest_buf.at[slot], rest_sem.at[slot]
    )


def accumulate(table, count_ref, head_ref, rest, pieces, sums, bufs, begin):
    fold_ref, gram_ref, extra_ref = sums
    buf, rest_buf, sem, rest_sem = bufs
    step = pl.program_id(0)
    slot = lax.rem(step, 2)
    count = count_ref[0]

    @pl.when(step == 0)
    def _():
        begin()
        fetch(table, count, rest, pieces, *bufs, 0, 0)

        @pl.when(count == 0)
        def _():
            rest_buf[...] = jnp.zeros_like(rest_buf)

    @pl.when(step + 1 < pl.num_programs(0))
    def _():
        fetch(table, count, rest, pieces, *bufs, step + 1, 1 - slot)

    pltpu.make_async_copy(pieces[0].at[pl.ds(0, buf.shape[1])], buf.at[slot], sem.at[slot]).wait()

    @pl.when(count > 0)
    def _():
        rest_copy(table, rest, rest_buf, rest_sem, step, slot, 0).wait()

    def listed(at):
        return jnp.concatenate([rest_buf[at, i] for i in range(STEP)], 1)

    t = buf[slot].reshape(256, STEP * LO)
    head = jnp.concatenate([head_ref[i] for i in range(STEP)], 1)
    fold_ref[...] += dot(head, t, NT)
    both = dot(jnp.concatenate([t, listed(slot)], 0), t, NT)
    gram_ref[...] += both[:256]
    extra_ref[:GROUP] += both[256:]

    def more(group, carry):
        copy = rest_copy(table, rest, rest_buf, rest_sem, step, slot, group)
        copy.start()
        copy.wait()
        at = pl.multiple_of(group * GROUP, GROUP)
        extra_ref[pl.ds(at, GROUP), :] += dot(listed(slot), buf[slot].reshape(256, STEP * LO), NT)
        return carry

    lax.fori_loop(1, groups_of(count), more, 0)


def first_kernel(
    table, count_ref, head_ref, rest, p0, p1, p2, p3, p4, fold_ref, gram_ref, extra_ref, *bufs
):
    sums = (fold_ref, gram_ref, extra_ref)

    def begin():
        for ref in sums:
            ref[...] = jnp.zeros_like(ref)

    accumulate(table, count_ref, head_ref, rest, (p0, p1, p2, p3, p4), sums, bufs, begin)


def second_kernel(
    table, count_ref, head_ref, rest, p0, p1, p2, p3, p4, fold_in, gram_in, extra_in,
    second_ref, owner_ref, list_ref, part_ref, gram_ref, fold_ref, extra_ref, *bufs,
):
    def begin():
        fold_ref[...] = fold_in[...]
        gram_ref[...] = gram_in[...]
        extra_ref[...] = extra_in[...]

    sums = (fold_ref, gram_ref, extra_ref)
    accumulate(table, count_ref, head_ref, rest, (p0, p1, p2, p3, p4), sums, bufs, begin)

    @pl.when(pl.program_id(0) == pl.num_programs(0) - 1)
    def _():
        n = owner_ref.shape[1]
        block = lax.broadcasted_iota(jnp.int32, (n, n), 0)
        place = lax.broadcasted_iota(jnp.int32, (n, n), 1)
        own = (block == list_ref[...]) & (place < count_ref[0])
        own = jnp.where(own, 1.0, 0.0).astype(BF)
        head, rest = halves(extra_ref[...])
        fold = fold_ref[...] + (dot(own, head, NN) + dot(own, rest, NN))
        head, rest = halves(second_ref[...].astype(F32) * fold)
        slot = lax.broadcasted_iota(jnp.int32, (part_ref.shape[0], n), 0)
        hot = (slot == owner_ref[...] - table[129]).astype(F32).astype(BF)
        part_ref[...] = dot(hot, head, NN) + dot(hot, rest, NN)


def product(table, count, head, rest, pieces, more, slab):
    n = head.shape[1]
    steps = HI // STEP // 2
    any_spec = pl.BlockSpec(memory_space=pl.ANY)
    whole = lambda x: pl.BlockSpec(x.shape, lambda i, *scalars: (0, 0))
    sums = [jax.ShapeDtypeStruct((rows, 256), F32) for rows in (n, 256, n)]
    out = [jax.ShapeDtypeStruct((slab, 256), F32), sums[1]] if more else sums
    scratch = [
        pltpu.VMEM((2, 8, *pieces[0].shape[1:]), BF),
        pltpu.VMEM((2, STEP, GROUP, LO), BF),
        pltpu.SemaphoreType.DMA((2,)),
        pltpu.SemaphoreType.DMA((2,)),
    ]
    if more:
        scratch = [pltpu.VMEM((n, 256), F32)] * 2 + scratch
    return pl.pallas_call(
        second_kernel if more else first_kernel,
        grid_spec=pltpu.PrefetchScalarGridSpec(
            num_scalar_prefetch=2,
            grid=(steps,),
            in_specs=[
                pl.BlockSpec((STEP, n, LO), lambda i, table, count: (2 * i + table[128], 0, 0))
            ]
            + [any_spec] * 6
            + [whole(x) for x in more],
            out_specs=[whole(x) for x in out],
            scratch_shapes=scratch,
        ),
        out_shape=out,
        cost_estimate=pl.CostEstimate(
            flops=15_000_000_000, bytes_accessed=30_000_000, transcendentals=0
        ),
    )(table, count, head, rest, *pieces, *more)


def exact(a, b, dims):
    return lax.dot_general(a, b, dims, precision=lax.Precision.HIGHEST, preferred_element_type=F32)


def inverse_kernel(gram_ref, out_ref, ok_ref, a_ref, x_ref, r_ref):
    n = gram_ref.shape[0]
    at_row = lax.broadcasted_iota(jnp.int32, (n, n), 0)
    at_col = lax.broadcasted_iota(jnp.int32, (n, n), 1)
    eye = jnp.where(at_row == at_col, 1.0, 0.0)
    gram = gram_ref[...]
    diagonal = gram * eye
    by_row = lax.rsqrt(jnp.sum(diagonal, 1, keepdims=True))
    by_col = lax.rsqrt(jnp.sum(diagonal, 0, keepdims=True))
    a = gram * by_row * by_col
    bound = jnp.max(jnp.sum(jnp.abs(a), 0, keepdims=True))
    start = jnp.where(bound < 1.9, 1.0, 1.0 / bound)
    a_ref[...] = a
    x_ref[...] = start * eye
    r_ref[...] = eye - start * a

    def size(r):
        return jnp.sqrt(jnp.sum(r * r))

    def unfinished(state):
        i, now, before = state
        stuck = (now < 0.3) & (now > 0.5 * before)
        return (now > TOLERANCE) & (i < 40) & jnp.logical_not(stuck)

    def improve(state):
        i, now, _ = state
        x = x_ref[...] + exact(x_ref[...], r_ref[...], NN)
        r = eye - exact(a_ref[...], x, NN)
        x_ref[...] = x
        r_ref[...] = r
        return i + 1, size(r), now

    last = lax.while_loop(unfinished, improve, (0, size(r_ref[...]), jnp.float32(1e30)))
    x = x_ref[...] + exact(x_ref[...], r_ref[...], NN)
    out_ref[...] = x * by_row * by_col
    ok_ref[0] = jnp.where(last[1] <= TOLERANCE, 1, 0)


def inverse(gram):
    n = gram.shape[0]
    made, ok = pl.pallas_call(
        inverse_kernel,
        out_shape=[jax.ShapeDtypeStruct((n, n), F32), jax.ShapeDtypeStruct((1,), jnp.int32)],
        out_specs=[
            pl.BlockSpec(memory_space=pltpu.VMEM),
            pl.BlockSpec(memory_space=pltpu.SMEM),
        ],
        scratch_shapes=[pltpu.VMEM((n, n), F32)] * 3,
        cost_estimate=pl.CostEstimate(
            flops=5_000_000_000, bytes_accessed=600_000, transcendentals=0
        ),
    )(gram)

    def by_factor():
        factor = jnp.linalg.cholesky(gram)
        return jax.scipy.linalg.cho_solve((factor, True), jnp.eye(n, dtype=F32))

    return lax.cond(ok[0] == 1, lambda: made, by_factor)


def solve_kernel(inverse_ref, spread_ref, out_ref):
    total = spread_ref[0]
    for i in range(1, spread_ref.shape[0]):
        total = total + spread_ref[i]
    out_ref[...] = exact(inverse_ref[...], total, NT).reshape(out_ref.shape)


def solve(inverted, spread):
    n, rows = inverted.shape[0], spread.shape[1]
    return pl.pallas_call(
        solve_kernel,
        out_shape=jax.ShapeDtypeStruct((n // 16, 16, rows), F32),
        cost_estimate=pl.CostEstimate(
            flops=500_000_000, bytes_accessed=1_500_000, transcendentals=0
        ),
    )(inverted, spread)


def per_device(
    block_values,
    block_length,
    block_owner,
    block_second,
    block_third,
    live_blocks,
    second_factor,
    third_factor,
):
    n_rows = lax.axis_size("rows")
    n_cols = lax.axis_size("cols")
    row_at = lax.axis_index("rows")
    col_at = lax.axis_index("cols")
    range_rows = second_factor.shape[0]
    slab = range_rows * n_cols // n_rows

    core = row_at & 1
    own, swapped, close, remote = gather_tables(third_factor.T, second_factor.T, core)
    spots = jnp.concatenate(
        [
            spot(jnp.arange(4, dtype=jnp.int32), row_at >> 1),
            jnp.stack([row_at >> 3, col_at * range_rows]),
        ]
    )
    picked, local_gram = pick(spots, close, remote, block_second[None, :])
    gram_second = summed_over_cols(local_gram)

    hi, lo, v, listed, count = prepare(block_third, block_values, block_length, live_blocks)
    head = build(hi, lo, v)
    rest = build_rest(count, listed, hi, lo, v)
    owner = block_owner[None, :]
    sums = product(piece_table(row_at, col_at, core, slab), count, head, rest, own, (), slab)
    part, gram_third = product(
        piece_table(row_at, col_at, 1 - core, slab),
        count,
        head,
        rest,
        swapped,
        (*sums, picked, owner, listed),
        slab,
    )

    gram = (gram_second / (range_rows * n_cols)) * (
        gram_third / (third_factor.shape[0] * n_cols)
    )
    spread = part.reshape(n_cols, slab // n_cols, -1)
    spread = lax.all_to_all(spread, "cols", 0, 0, tiled=True)
    solved = solve(inverse(gram), spread)
    moved = lax.all_to_all(solved, "rows", 0, 0, tiled=True)
    share = n_rows // n_cols
    moved = moved.reshape(n_cols, share, *solved.shape[1:])
    moved = lax.all_to_all(moved, "cols", 0, 0, tiled=True)
    return moved.transpose(1, 0, 3, 2).reshape(range_rows, solved.shape[1])


def solution(mesh):
    return jax.shard_map(
        per_device,
        mesh=mesh,
        in_specs=(
            P(("rows", "cols"), None),
            P(("rows", "cols")),
            P(("rows", "cols")),
            P(("rows", "cols")),
            P(("rows", "cols"), None),
            P(("rows", "cols")),
            P("cols", "rows"),
            P("cols", "rows"),
        ),
        out_specs=P("cols", "rows"),
        check_vma=False,
    )
```

```python
import functools

import jax
import jax.numpy as jnp
from jax import lax
from jax.experimental import pallas as pl
from jax.experimental.pallas import tpu as pltpu
from jax.sharding import PartitionSpec as P


BF = jnp.bfloat16
F32 = jnp.float32
NT = (((1,), (1,)), ((), ()))
NN = (((1,), (0,)), ((), ()))

LO = 256
HI = 128
NB = 16
PITCH = 140
GROUP = 64
PARTS = 4
STEP = 8
TOLERANCE = 3e-4
AXES = ("rows", "cols")
SHIFTS = (1, -1, 2)


def dot(a, b, dims):
    return lax.dot_general(a, b, dims, preferred_element_type=F32)


def halves(x):
    head = x.astype(BF)
    return head, (x - head.astype(F32)).astype(BF)


def prepare_kernel(
    live_ref, third_ref, value_ref, length_ref, hi_ref, lo_ref, v_ref, list_ref, count_ref, again
):
    step = pl.program_id(0)
    n, width = third_ref.shape
    third = third_ref[...]
    lane = lax.broadcasted_iota(jnp.int32, (n, width), 1)
    block = lax.broadcasted_iota(jnp.int32, (n, width), 0) + step * n
    across = lax.broadcasted_iota(jnp.int32, (n, width), 0) == lane
    length = jnp.sum(jnp.where(across, length_ref[...].astype(F32), 0.0), 1, keepdims=True)
    live = (lane.astype(F32) < length) & (block < live_ref[0])
    hi_ref[...] = (third >> 8).astype(F32)
    lo_ref[...] = (third & (LO - 1)).astype(F32)
    v_ref[...] = jnp.where(live, value_ref[...].astype(F32), 0.0)
    marked = jnp.where(live, third, (1 << 15) + lane)
    pair = marked[: n // 2] | (marked[n // 2 :] << 16)
    low = jnp.zeros_like(pair)
    high = jnp.zeros_like(pair)
    for shift in range(1, width // 2 + 1):
        differ = pair ^ pltpu.roll(pair, shift, 1)
        low = low | ((differ & 0xFFFF) - 1)
        high = high | (lax.shift_right_logical(differ, 16) - 1)
    same = jnp.concatenate([jnp.where(x < 0, 1.0, 0.0) for x in (low, high)], 0)
    found = jnp.max(same, 1, keepdims=True)
    again[pl.ds(pl.multiple_of(step * n, n), n), :] = jnp.broadcast_to(found, (n, width))

    @pl.when(step == pl.num_programs(0) - 1)
    def _():
        total = again.shape[0]
        flags = again[...]
        row = lax.broadcasted_iota(jnp.int32, (total, total), 0)
        col = lax.broadcasted_iota(jnp.int32, (total, total), 1)
        earlier = jnp.where(col < row, 1.0, 0.0).astype(BF)
        ahead = dot(earlier, flags.astype(BF), NN)
        wide = jnp.concatenate([ahead] * (total // width), 1)
        on = jnp.concatenate([flags] * (total // width), 1)
        mine = (on > 0.5) & (wide == col.astype(F32))
        picked = jnp.sum(jnp.where(mine, row.astype(F32), 0.0), 0, keepdims=True)
        list_ref[...] = picked.astype(jnp.int32)
        count_ref[0] = jnp.sum(flags[:, :1]).astype(jnp.int32)


def prepare(third, values, length, live):
    n, width = third.shape
    rows = 128
    spec = pl.BlockSpec((rows, width), lambda i: (i, 0))
    shape = jax.ShapeDtypeStruct((n, width), F32)
    return pl.pallas_call(
        prepare_kernel,
        grid=(n // rows,),
        in_specs=[
            pl.BlockSpec(memory_space=pltpu.SMEM),
            spec,
            spec,
            pl.BlockSpec((1, rows), lambda i: (0, i)),
        ],
        out_specs=[spec] * 3
        + [pl.BlockSpec((1, n), lambda i: (0, 0)), pl.BlockSpec(memory_space=pltpu.SMEM)],
        out_shape=[shape] * 3
        + [jax.ShapeDtypeStruct((1, n), jnp.int32), jax.ShapeDtypeStruct((1,), jnp.int32)],
        scratch_shapes=[pltpu.VMEM((n, width), F32)],
        cost_estimate=pl.CostEstimate(
            flops=3_000_000_000, bytes_accessed=1_000_000, transcendentals=0
        ),
    )(live, third, values, length[None, :])


def spread_blocks(rows_of, left, right):
    base = lax.broadcasted_iota(jnp.int32, (16, 128), 0)
    iota = [(base + 16 * j).astype(F32).astype(BF) for j in range(LO // 16)]
    one = jnp.ones((16, 128), BF)
    zero = jnp.zeros((16, 128), BF)
    for b in range(NB):
        hi, lo, v = (jnp.broadcast_to(row, (16, 128)).astype(BF) for row in rows_of(b))
        a = jnp.concatenate([jnp.where(hi == iota[j], v, zero) for j in range(HI // 16)], 0)
        c = jnp.concatenate([jnp.where(lo == iota[j], one, zero) for j in range(LO // 16)], 0)
        s = dot(a, c, NT)
        left[b * PITCH : b * PITCH + HI, :] = s[:, :128]
        right[b * PITCH : b * PITCH + HI, :] = s[:, 128:]


def write_blocks(left, right, buf, out_ref, at, sem, value_of):
    quarter = HI // 4
    for q in range(4):

        def some(i, carry, q=q):
            for u in range(16):
                h = q * quarter + i * 16 + u
                blocks = pl.ds(h, NB, stride=PITCH)
                buf[h] = value_of(jnp.concatenate([left[blocks, :], right[blocks, :]], 1))
            return carry

        lax.fori_loop(0, quarter // 16, some, 0)
        rows = pl.ds(q * quarter, quarter)
        pltpu.make_async_copy(buf.at[rows], out_ref.at[rows, pl.ds(at, NB), :], sem).start()


def written(buf, out_ref, sem):
    return pltpu.make_async_copy(buf, out_ref.at[:, pl.ds(0, NB), :], sem)


def build_kernel(first, hi_ref, lo_ref, v_ref, *refs):
    head_ref, left, right, buf, sem = refs[-5:]
    step = pl.program_id(0)
    slot = lax.rem(step, 2)
    spread_blocks(
        lambda b: [ref[b : b + 1, :] for ref in (hi_ref, lo_ref, v_ref)], left, right
    )

    @pl.when(step >= 2)
    def _():
        written(buf.at[slot], head_ref, sem.at[slot]).wait()

    at = pl.multiple_of((first + step) * NB, NB)
    write_blocks(
        left, right, buf.at[slot], head_ref, at, sem.at[slot], lambda x: x.astype(BF)
    )

    @pl.when(step == pl.num_programs(0) - 1)
    def _():
        for i in range(2):
            written(buf.at[i], head_ref, sem.at[i]).wait()


def build(hi, lo, v):
    n = hi.shape[0]
    steps = n // NB // PARTS
    made = ()
    for part in range(PARTS):
        first = part * steps
        spec = pl.BlockSpec((NB, 128), lambda i, first=first: (first + i, 0))
        call = pl.pallas_call(
            functools.partial(build_kernel, first),
            grid=(steps,),
            in_specs=[spec] * 3 + [pl.BlockSpec(memory_space=pl.ANY)] * len(made),
            out_specs=pl.BlockSpec(memory_space=pl.ANY),
            out_shape=jax.ShapeDtypeStruct((HI, n, LO), BF),
            scratch_shapes=[pltpu.VMEM((NB * PITCH, 128), F32)] * 2
            + [pltpu.VMEM((2, HI, NB, LO), BF), pltpu.SemaphoreType.DMA((2,))],
            input_output_aliases={3: 0} if made else {},
            cost_estimate=pl.CostEstimate(
                flops=30_000_000_000 // PARTS,
                bytes_accessed=n * HI * LO * 2 // PARTS,
                transcendentals=0,
            ),
        )
        made = (call(hi, lo, v, *made),)
    return made[0]


def groups_of(count):
    return (count + GROUP - 1) // GROUP


def rest_kernel(count_ref, list_ref, hi_ref, lo_ref, v_ref, rest_ref, left, right, buf, sem):
    count = count_ref[0]

    def some(i, carry):
        def rows_of(b):
            slot = i * NB + b
            block = list_ref[0, slot]
            on = jnp.where(slot < count, 1.0, 0.0).astype(F32)
            hi, lo, v = (ref[pl.ds(block, 1), :] for ref in (hi_ref, lo_ref, v_ref))
            return hi, lo, v * on

        spread_blocks(rows_of, left, right)

        @pl.when(i > 0)
        def _():
            written(buf, rest_ref, sem).wait()

        at = pl.multiple_of(i * NB, NB)
        write_blocks(
            left, right, buf, rest_ref, at, sem, lambda x: (x - x.astype(BF).astype(F32)).astype(BF)
        )
        return carry

    lax.fori_loop(0, groups_of(count) * (GROUP // NB), some, 0)

    @pl.when(count > 0)
    def _():
        written(buf, rest_ref, sem).wait()


def build_rest(count, listed, hi, lo, v):
    n = hi.shape[0]
    return pl.pallas_call(
        rest_kernel,
        in_specs=[pl.BlockSpec(memory_space=pltpu.SMEM)] * 2
        + [pl.BlockSpec(memory_space=pltpu.VMEM)] * 3,
        out_specs=pl.BlockSpec(memory_space=pl.ANY),
        out_shape=jax.ShapeDtypeStruct((HI, n, LO), BF),
        scratch_shapes=[pltpu.VMEM((NB * PITCH, 128), F32)] * 2
        + [pltpu.VMEM((HI, NB, LO), BF), pltpu.SemaphoreType.DMA],
        cost_estimate=pl.CostEstimate(
            flops=6_000_000_000, bytes_accessed=6_000_000, transcendentals=0
        ),
    )(count, listed, hi, lo, v)


def place(i):
    return {
        "x": i // 16 % 4,
        "y": i // 2 % 4,
        "z": i // 64 * 2 + i % 2,
        "core": i // 8 % 2,
    }


def device(at):
    return (((at["z"] // 2 * 4 + at["x"]) * 2 + at["core"]) * 4 + at["y"]) * 2 + at["z"] % 2


def shifted(value, dims, shift):
    pairs = []
    for i in range(128):
        at = place(i)
        dim = dims[at["core"]]
        at[dim] = (at[dim] + shift) % (2 if dim == "core" else 4)
        pairs.append((i, device(at)))
    return lax.ppermute(value, AXES, pairs)


def across(value):
    return shifted(value, ("core", "core"), 1)


def ring(value, dims):
    came = [value]
    for shift in SHIFTS:
        came.append(shifted(value, dims, shift))
    return jnp.concatenate(came, 0)


def summed_over_cols(value):
    for dim, bit in (("z", 1), ("y", 1), ("y", 2)):
        pairs = []
        for j in range(128):
            at = place(j)
            at[dim] ^= bit
            pairs.append((j, device(at)))
        other = lax.ppermute(value, AXES, pairs)
        value = value + other
    return value


def gather_table(piece, core):
    half = piece.shape[1] // 2
    mine = lax.dynamic_slice_in_dim(piece, core * half, half, 1)
    other = lax.dynamic_slice_in_dim(piece, (1 - core) * half, half, 1)
    came = across(other)
    unit = jnp.where(core == 0, jnp.stack([mine, came]), jnp.stack([came, mine]))
    near = ring(unit[None], ("x", "y"))
    plane = ring(near[None], ("y", "z"))
    last = ("z", "x")
    left = shifted(plane, last, 1)
    right = shifted(plane, last, -1)
    far0 = shifted(left[:2], last, 1)
    far1 = shifted(right[2:], last, -1)
    own = [x.reshape(-1, *unit.shape) for x in (plane, left, right, far0, far1)]
    return own, [across(x) for x in own]


def spot(there, here):
    ahead = (there - here) & 3
    return jnp.where(ahead == 3, 1, jnp.where(ahead == 0, 0, ahead + 1))


def pick_kernel(first_ref, range_ref, index_ref, picked_ref, gram_ref):
    r = range_ref[...].reshape(256, range_ref.shape[2])
    gram_ref[...] = dot(r, r, NT)
    at = lax.broadcasted_iota(jnp.int32, (r.shape[1], index_ref.shape[1]), 0)
    hot = (at == index_ref[...] - first_ref[0]).astype(F32).astype(BF)
    picked_ref[...] = dot(r, hot, NN).T.astype(BF)


def pick(first, second_range, index):
    n = index.shape[1]
    return pl.pallas_call(
        pick_kernel,
        in_specs=[pl.BlockSpec(memory_space=pltpu.SMEM)]
        + [pl.BlockSpec(memory_space=pltpu.VMEM)] * 2,
        out_specs=[pl.BlockSpec(memory_space=pltpu.VMEM)] * 2,
        out_shape=[jax.ShapeDtypeStruct((n, 256), BF), jax.ShapeDtypeStruct((256, 256), F32)],
        cost_estimate=pl.CostEstimate(
            flops=2_000_000_000, bytes_accessed=2_000_000, transcendentals=0
        ),
    )(first, second_range, index)


def piece_table(row_at, col_at, order, slab):
    y, z_lo, z_hi, x = jnp.meshgrid(
        jnp.arange(4), jnp.arange(2), jnp.arange(2), jnp.arange(4), indexing="ij"
    )
    at_x = spot(x, row_at >> 1)
    at_y = spot(y, col_at >> 1)
    at_z = spot(z_hi * 2 + z_lo, (row_at >> 3) * 2 + (col_at & 1))
    first = jnp.where(order == 0, at_x, at_y)
    second = jnp.where(order == 0, at_y, at_z)
    third = jnp.where(order == 0, at_z, at_x)
    late = (third == 3) & (second >= 2)
    array = third + late
    index = (second - 2 * late) * 4 + first
    last = jnp.stack([order, row_at * slab])
    return jnp.concatenate([array.ravel(), index.ravel(), last]).astype(jnp.int32)


def fetch(table, count, rest, pieces, buf, rest_buf, sem, rest_sem, step, slot):
    n = buf.shape[1]
    for p in range(n):
        array = table[step * n + p]
        index = table[64 + step * n + p]
        for a, ref in enumerate(pieces):

            @pl.when(array == a)
            def _(ref=ref, p=p):
                pltpu.make_async_copy(ref.at[index], buf.at[slot, p], sem.at[slot]).start()

    @pl.when(count > 0)
    def _():
        rest_copy(table, rest, rest_buf, rest_sem, step, slot, 0).start()


def rest_copy(table, rest, rest_buf, rest_sem, step, slot, group):
    first = pl.multiple_of((2 * step + table[128]) * STEP, STEP)
    at = pl.multiple_of(group * GROUP, GROUP)
    return pltpu.make_async_copy(
        rest.at[pl.ds(first, STEP), pl.ds(at, GROUP), :], rest_buf.at[slot], rest_sem.at[slot]
    )


def accumulate(table, count_ref, head_ref, rest, pieces, sums, bufs, begin):
    fold_ref, gram_ref, extra_ref = sums
    buf, rest_buf, sem, rest_sem = bufs
    step = pl.program_id(0)
    slot = lax.rem(step, 2)
    count = count_ref[0]

    @pl.when(step == 0)
    def _():
        begin()
        fetch(table, count, rest, pieces, *bufs, 0, 0)

        @pl.when(count == 0)
        def _():
            rest_buf[...] = jnp.zeros_like(rest_buf)

    @pl.when(step + 1 < pl.num_programs(0))
    def _():
        fetch(table, count, rest, pieces, *bufs, step + 1, 1 - slot)

    pltpu.make_async_copy(pieces[0].at[pl.ds(0, buf.shape[1])], buf.at[slot], sem.at[slot]).wait()

    @pl.when(count > 0)
    def _():
        rest_copy(table, rest, rest_buf, rest_sem, step, slot, 0).wait()

    def listed(at):
        return jnp.concatenate([rest_buf[at, i] for i in range(STEP)], 1)

    t = buf[slot].reshape(256, STEP * LO)
    head = jnp.concatenate([head_ref[i] for i in range(STEP)], 1)
    fold_ref[...] += dot(head, t, NT)
    both = dot(jnp.concatenate([t, listed(slot)], 0), t, NT)
    gram_ref[...] += both[:256]
    extra_ref[:GROUP] += both[256:]

    def more(group, carry):
        copy = rest_copy(table, rest, rest_buf, rest_sem, step, slot, group)
        copy.start()
        copy.wait()
        at = pl.multiple_of(group * GROUP, GROUP)
        extra_ref[pl.ds(at, GROUP), :] += dot(listed(slot), buf[slot].reshape(256, STEP * LO), NT)
        return carry

    lax.fori_loop(1, groups_of(count), more, 0)


def first_kernel(
    table, count_ref, head_ref, rest, p0, p1, p2, p3, p4, fold_ref, gram_ref, extra_ref, *bufs
):
    sums = (fold_ref, gram_ref, extra_ref)

    def begin():
        for ref in sums:
            ref[...] = jnp.zeros_like(ref)

    accumulate(table, count_ref, head_ref, rest, (p0, p1, p2, p3, p4), sums, bufs, begin)


def second_kernel(
    table, count_ref, head_ref, rest, p0, p1, p2, p3, p4, fold_in, gram_in, extra_in,
    second_ref, owner_ref, list_ref, part_ref, gram_ref, fold_ref, extra_ref, *bufs,
):
    def begin():
        fold_ref[...] = fold_in[...]
        gram_ref[...] = gram_in[...]
        extra_ref[...] = extra_in[...]

    sums = (fold_ref, gram_ref, extra_ref)
    accumulate(table, count_ref, head_ref, rest, (p0, p1, p2, p3, p4), sums, bufs, begin)

    @pl.when(pl.program_id(0) == pl.num_programs(0) - 1)
    def _():
        n = owner_ref.shape[1]
        block = lax.broadcasted_iota(jnp.int32, (n, n), 0)
        place = lax.broadcasted_iota(jnp.int32, (n, n), 1)
        own = (block == list_ref[...]) & (place < count_ref[0])
        own = jnp.where(own, 1.0, 0.0).astype(BF)
        head, rest = halves(extra_ref[...])
        fold = fold_ref[...] + (dot(own, head, NN) + dot(own, rest, NN))
        head, rest = halves(second_ref[...].astype(F32) * fold)
        slot = lax.broadcasted_iota(jnp.int32, (part_ref.shape[0], n), 0)
        hot = (slot == owner_ref[...] - table[129]).astype(F32).astype(BF)
        part_ref[...] = dot(hot, head, NN) + dot(hot, rest, NN)


def product(table, count, head, rest, pieces, more, slab):
    n = head.shape[1]
    steps = HI // STEP // 2
    any_spec = pl.BlockSpec(memory_space=pl.ANY)
    whole = lambda x: pl.BlockSpec(x.shape, lambda i, *scalars: (0, 0))
    sums = [jax.ShapeDtypeStruct((rows, 256), F32) for rows in (n, 256, n)]
    out = [jax.ShapeDtypeStruct((slab, 256), F32), sums[1]] if more else sums
    scratch = [
        pltpu.VMEM((2, 8, *pieces[0].shape[1:]), BF),
        pltpu.VMEM((2, STEP, GROUP, LO), BF),
        pltpu.SemaphoreType.DMA((2,)),
        pltpu.SemaphoreType.DMA((2,)),
    ]
    if more:
        scratch = [pltpu.VMEM((n, 256), F32)] * 2 + scratch
    return pl.pallas_call(
        second_kernel if more else first_kernel,
        grid_spec=pltpu.PrefetchScalarGridSpec(
            num_scalar_prefetch=2,
            grid=(steps,),
            in_specs=[
                pl.BlockSpec((STEP, n, LO), lambda i, table, count: (2 * i + table[128], 0, 0))
            ]
            + [any_spec] * 6
            + [whole(x) for x in more],
            out_specs=[whole(x) for x in out],
            scratch_shapes=scratch,
        ),
        out_shape=out,
        cost_estimate=pl.CostEstimate(
            flops=15_000_000_000, bytes_accessed=30_000_000, transcendentals=0
        ),
    )(table, count, head, rest, *pieces, *more)


def exact(a, b, dims):
    return lax.dot_general(a, b, dims, precision=lax.Precision.HIGHEST, preferred_element_type=F32)


def inverse_kernel(gram_ref, out_ref, ok_ref, a_ref, x_ref, r_ref):
    n = gram_ref.shape[0]
    at_row = lax.broadcasted_iota(jnp.int32, (n, n), 0)
    at_col = lax.broadcasted_iota(jnp.int32, (n, n), 1)
    eye = jnp.where(at_row == at_col, 1.0, 0.0)
    gram = gram_ref[...]
    diagonal = gram * eye
    by_row = lax.rsqrt(jnp.sum(diagonal, 1, keepdims=True))
    by_col = lax.rsqrt(jnp.sum(diagonal, 0, keepdims=True))
    a = gram * by_row * by_col
    bound = jnp.max(jnp.sum(jnp.abs(a), 0, keepdims=True))
    start = jnp.where(bound < 1.9, 1.0, 1.0 / bound)
    a_ref[...] = a
    x_ref[...] = start * eye
    r_ref[...] = eye - start * a

    def size(r):
        return jnp.sqrt(jnp.sum(r * r))

    def unfinished(state):
        i, now, before = state
        stuck = (now < 0.3) & (now > 0.5 * before)
        return (now > TOLERANCE) & (i < 40) & jnp.logical_not(stuck)

    def improve(state):
        i, now, _ = state
        x = x_ref[...] + exact(x_ref[...], r_ref[...], NN)
        r = eye - exact(a_ref[...], x, NN)
        x_ref[...] = x
        r_ref[...] = r
        return i + 1, size(r), now

    last = lax.while_loop(unfinished, improve, (0, size(r_ref[...]), jnp.float32(1e30)))
    x = x_ref[...] + exact(x_ref[...], r_ref[...], NN)
    out_ref[...] = x * by_row * by_col
    ok_ref[0] = jnp.where(last[1] <= TOLERANCE, 1, 0)


def inverse(gram):
    n = gram.shape[0]
    made, ok = pl.pallas_call(
        inverse_kernel,
        out_shape=[jax.ShapeDtypeStruct((n, n), F32), jax.ShapeDtypeStruct((1,), jnp.int32)],
        out_specs=[
            pl.BlockSpec(memory_space=pltpu.VMEM),
            pl.BlockSpec(memory_space=pltpu.SMEM),
        ],
        scratch_shapes=[pltpu.VMEM((n, n), F32)] * 3,
        cost_estimate=pl.CostEstimate(
            flops=5_000_000_000, bytes_accessed=600_000, transcendentals=0
        ),
    )(gram)

    def by_factor():
        factor = jnp.linalg.cholesky(gram)
        return jax.scipy.linalg.cho_solve((factor, True), jnp.eye(n, dtype=F32))

    return lax.cond(ok[0] == 1, lambda: made, by_factor)


def solve_kernel(inverse_ref, spread_ref, out_ref):
    total = spread_ref[0]
    for i in range(1, spread_ref.shape[0]):
        total = total + spread_ref[i]
    out_ref[...] = exact(inverse_ref[...], total, NT).reshape(out_ref.shape)


def solve(inverted, spread):
    n, rows = inverted.shape[0], spread.shape[1]
    return pl.pallas_call(
        solve_kernel,
        out_shape=jax.ShapeDtypeStruct((n // 16, 16, rows), F32),
        cost_estimate=pl.CostEstimate(
            flops=500_000_000, bytes_accessed=1_500_000, transcendentals=0
        ),
    )(inverted, spread)


def per_device(
    block_values,
    block_length,
    block_owner,
    block_second,
    block_third,
    live_blocks,
    second_factor,
    third_factor,
):
    n_rows = lax.axis_size("rows")
    n_cols = lax.axis_size("cols")
    row_at = lax.axis_index("rows")
    col_at = lax.axis_index("cols")
    range_rows = second_factor.shape[0]
    slab = range_rows * n_cols // n_rows

    core = row_at & 1
    own, swapped = gather_table(third_factor.T, core)
    second = jnp.broadcast_to(second_factor.T[None], (n_rows, *second_factor.T.shape))
    second_range = lax.all_to_all(second, "rows", 0, 0, tiled=True)
    picked, local_gram = pick(
        (col_at * range_rows)[None], second_range, block_second[None, :]
    )
    gram_second = summed_over_cols(local_gram)

    hi, lo, v, listed, count = prepare(block_third, block_values, block_length, live_blocks)
    head = build(hi, lo, v)
    rest = build_rest(count, listed, hi, lo, v)
    owner = block_owner[None, :]
    sums = product(piece_table(row_at, col_at, core, slab), count, head, rest, own, (), slab)
    part, gram_third = product(
        piece_table(row_at, col_at, 1 - core, slab),
        count,
        head,
        rest,
        swapped,
        (*sums, picked, owner, listed),
        slab,
    )

    gram = (gram_second / (range_rows * n_cols)) * (
        gram_third / (third_factor.shape[0] * n_cols)
    )
    spread = part.reshape(n_cols, slab // n_cols, -1)
    spread = lax.all_to_all(spread, "cols", 0, 0, tiled=True)
    solved = solve(inverse(gram), spread)
    moved = lax.all_to_all(solved, "rows", 0, 0, tiled=True)
    share = n_rows // n_cols
    moved = moved.reshape(n_cols, share, *solved.shape[1:])
    moved = lax.all_to_all(moved, "cols", 0, 0, tiled=True)
    return moved.transpose(1, 0, 3, 2).reshape(range_rows, solved.shape[1])


def solution(mesh):
    return jax.shard_map(
        per_device,
        mesh=mesh,
        in_specs=(
            P(("rows", "cols"), None),
            P(("rows", "cols")),
            P(("rows", "cols")),
            P(("rows", "cols")),
            P(("rows", "cols"), None),
            P(("rows", "cols")),
            P("cols", "rows"),
            P("cols", "rows"),
        ),
        out_specs=P("cols", "rows"),
        check_vma=False,
    )
```

```python
import functools

import jax
import jax.numpy as jnp
from jax import lax
from jax.experimental import pallas as pl
from jax.experimental.pallas import tpu as pltpu
from jax.sharding import PartitionSpec as P


BF = jnp.bfloat16
F32 = jnp.float32
NT = (((1,), (1,)), ((), ()))
NN = (((1,), (0,)), ((), ()))

LO = 256
HI = 128
NB = 16
PITCH = 140
GROUP = 64
PARTS = 4
STEP = 8
CHUNK = 2
TOLERANCE = 3e-4
AXES = ("rows", "cols")
SHIFTS = (1, -1, 2)


def dot(a, b, dims):
    return lax.dot_general(a, b, dims, preferred_element_type=F32)


def halves(x):
    head = x.astype(BF)
    return head, (x - head.astype(F32)).astype(BF)


def prepare_kernel(
    live_ref, third_ref, value_ref, length_ref, hi_ref, lo_ref, v_ref, list_ref, count_ref, again
):
    step = pl.program_id(0)
    n, width = third_ref.shape
    third = third_ref[...]
    lane = lax.broadcasted_iota(jnp.int32, (n, width), 1)
    block = lax.broadcasted_iota(jnp.int32, (n, width), 0) + step * n
    across = lax.broadcasted_iota(jnp.int32, (n, width), 0) == lane
    length = jnp.sum(jnp.where(across, length_ref[...].astype(F32), 0.0), 1, keepdims=True)
    live = (lane.astype(F32) < length) & (block < live_ref[0])
    hi_ref[...] = (third >> 8).astype(F32)
    lo_ref[...] = (third & (LO - 1)).astype(F32)
    v_ref[...] = jnp.where(live, value_ref[...].astype(F32), 0.0)
    marked = jnp.where(live, third, (1 << 15) + lane)
    pair = marked[: n // 2] | (marked[n // 2 :] << 16)
    low = jnp.zeros_like(pair)
    high = jnp.zeros_like(pair)
    for shift in range(1, width // 2 + 1):
        differ = pair ^ pltpu.roll(pair, shift, 1)
        low = low | ((differ & 0xFFFF) - 1)
        high = high | (lax.shift_right_logical(differ, 16) - 1)
    same = jnp.concatenate([jnp.where(x < 0, 1.0, 0.0) for x in (low, high)], 0)
    found = jnp.max(same, 1, keepdims=True)
    again[pl.ds(pl.multiple_of(step * n, n), n), :] = jnp.broadcast_to(found, (n, width))

    @pl.when(step == pl.num_programs(0) - 1)
    def _():
        total = again.shape[0]
        flags = again[...]
        row = lax.broadcasted_iota(jnp.int32, (total, total), 0)
        col = lax.broadcasted_iota(jnp.int32, (total, total), 1)
        earlier = jnp.where(col < row, 1.0, 0.0).astype(BF)
        ahead = dot(earlier, flags.astype(BF), NN)
        wide = jnp.concatenate([ahead] * (total // width), 1)
        on = jnp.concatenate([flags] * (total // width), 1)
        mine = (on > 0.5) & (wide == col.astype(F32))
        picked = jnp.sum(jnp.where(mine, row.astype(F32), 0.0), 0, keepdims=True)
        list_ref[...] = picked.astype(jnp.int32)
        count_ref[0] = jnp.sum(flags[:, :1]).astype(jnp.int32)


def prepare(third, values, length, live):
    n, width = third.shape
    rows = 128
    spec = pl.BlockSpec((rows, width), lambda i: (i, 0))
    shape = jax.ShapeDtypeStruct((n, width), F32)
    return pl.pallas_call(
        prepare_kernel,
        grid=(n // rows,),
        in_specs=[
            pl.BlockSpec(memory_space=pltpu.SMEM),
            spec,
            spec,
            pl.BlockSpec((1, rows), lambda i: (0, i)),
        ],
        out_specs=[spec] * 3
        + [pl.BlockSpec((1, n), lambda i: (0, 0)), pl.BlockSpec(memory_space=pltpu.SMEM)],
        out_shape=[shape] * 3
        + [jax.ShapeDtypeStruct((1, n), jnp.int32), jax.ShapeDtypeStruct((1,), jnp.int32)],
        scratch_shapes=[pltpu.VMEM((n, width), F32)],
        cost_estimate=pl.CostEstimate(
            flops=3_000_000_000, bytes_accessed=1_000_000, transcendentals=0
        ),
    )(live, third, values, length[None, :])


def spread_blocks(rows_of, left, right):
    base = lax.broadcasted_iota(jnp.int32, (16, 128), 0)
    iota = [(base + 16 * j).astype(F32).astype(BF) for j in range(LO // 16)]
    one = jnp.ones((16, 128), BF)
    zero = jnp.zeros((16, 128), BF)
    for b in range(NB):
        hi, lo, v = (jnp.broadcast_to(row, (16, 128)).astype(BF) for row in rows_of(b))
        a = jnp.concatenate([jnp.where(hi == iota[j], v, zero) for j in range(HI // 16)], 0)
        c = jnp.concatenate([jnp.where(lo == iota[j], one, zero) for j in range(LO // 16)], 0)
        s = dot(a, c, NT)
        left[b * PITCH : b * PITCH + HI, :] = s[:, :128]
        right[b * PITCH : b * PITCH + HI, :] = s[:, 128:]


def write_blocks(left, right, buf, out_ref, at, sem, value_of):
    quarter = HI // 4
    for q in range(4):

        def some(i, carry, q=q):
            for u in range(16):
                h = q * quarter + i * 16 + u
                blocks = pl.ds(h, NB, stride=PITCH)
                buf[h] = value_of(jnp.concatenate([left[blocks, :], right[blocks, :]], 1))
            return carry

        lax.fori_loop(0, quarter // 16, some, 0)
        rows = pl.ds(q * quarter, quarter)
        pltpu.make_async_copy(buf.at[rows], out_ref.at[rows, pl.ds(at, NB), :], sem).start()


def written(buf, out_ref, sem):
    return pltpu.make_async_copy(buf, out_ref.at[:, pl.ds(0, NB), :], sem)


def build_kernel(first, hi_ref, lo_ref, v_ref, *refs):
    head_ref, left, right, buf, sem = refs[-5:]
    step = pl.program_id(0)
    slot = lax.rem(step, 2)
    spread_blocks(
        lambda b: [ref[b : b + 1, :] for ref in (hi_ref, lo_ref, v_ref)], left, right
    )

    @pl.when(step >= 2)
    def _():
        written(buf.at[slot], head_ref, sem.at[slot]).wait()

    at = pl.multiple_of((first + step) * NB, NB)
    write_blocks(
        left, right, buf.at[slot], head_ref, at, sem.at[slot], lambda x: x.astype(BF)
    )

    @pl.when(step == pl.num_programs(0) - 1)
    def _():
        for i in range(2):
            written(buf.at[i], head_ref, sem.at[i]).wait()


def build(hi, lo, v):
    n = hi.shape[0]
    steps = n // NB // PARTS
    made = ()
    for part in range(PARTS):
        first = part * steps
        spec = pl.BlockSpec((NB, 128), lambda i, first=first: (first + i, 0))
        call = pl.pallas_call(
            functools.partial(build_kernel, first),
            grid=(steps,),
            in_specs=[spec] * 3 + [pl.BlockSpec(memory_space=pl.ANY)] * len(made),
            out_specs=pl.BlockSpec(memory_space=pl.ANY),
            out_shape=jax.ShapeDtypeStruct((HI, n, LO), BF),
            scratch_shapes=[pltpu.VMEM((NB * PITCH, 128), F32)] * 2
            + [pltpu.VMEM((2, HI, NB, LO), BF), pltpu.SemaphoreType.DMA((2,))],
            input_output_aliases={3: 0} if made else {},
            cost_estimate=pl.CostEstimate(
                flops=30_000_000_000 // PARTS,
                bytes_accessed=n * HI * LO * 2 // PARTS,
                transcendentals=0,
            ),
        )
        made = (call(hi, lo, v, *made),)
    return made[0]


def groups_of(count):
    return (count + GROUP - 1) // GROUP


def rest_kernel(count_ref, list_ref, hi_ref, lo_ref, v_ref, rest_ref, left, right, buf, sem):
    count = count_ref[0]

    def some(i, carry):
        def rows_of(b):
            slot = i * NB + b
            block = list_ref[0, slot]
            on = jnp.where(slot < count, 1.0, 0.0).astype(F32)
            hi, lo, v = (ref[pl.ds(block, 1), :] for ref in (hi_ref, lo_ref, v_ref))
            return hi, lo, v * on

        spread_blocks(rows_of, left, right)

        @pl.when(i > 0)
        def _():
            written(buf, rest_ref, sem).wait()

        at = pl.multiple_of(i * NB, NB)
        write_blocks(
            left, right, buf, rest_ref, at, sem, lambda x: (x - x.astype(BF).astype(F32)).astype(BF)
        )
        return carry

    lax.fori_loop(0, groups_of(count) * (GROUP // NB), some, 0)

    @pl.when(count > 0)
    def _():
        written(buf, rest_ref, sem).wait()


def build_rest(count, listed, hi, lo, v):
    n = hi.shape[0]
    return pl.pallas_call(
        rest_kernel,
        in_specs=[pl.BlockSpec(memory_space=pltpu.SMEM)] * 2
        + [pl.BlockSpec(memory_space=pltpu.VMEM)] * 3,
        out_specs=pl.BlockSpec(memory_space=pl.ANY),
        out_shape=jax.ShapeDtypeStruct((HI, n, LO), BF),
        scratch_shapes=[pltpu.VMEM((NB * PITCH, 128), F32)] * 2
        + [pltpu.VMEM((HI, NB, LO), BF), pltpu.SemaphoreType.DMA],
        cost_estimate=pl.CostEstimate(
            flops=6_000_000_000, bytes_accessed=6_000_000, transcendentals=0
        ),
    )(count, listed, hi, lo, v)


def place(i):
    return {
        "x": i // 16 % 4,
        "y": i // 2 % 4,
        "z": i // 64 * 2 + i % 2,
        "core": i // 8 % 2,
    }


def device(at):
    return (((at["z"] // 2 * 4 + at["x"]) * 2 + at["core"]) * 4 + at["y"]) * 2 + at["z"] % 2


def shifted(value, dims, shift):
    pairs = []
    for i in range(128):
        at = place(i)
        dim = dims[at["core"]]
        at[dim] = (at[dim] + shift) % (2 if dim == "core" else 4)
        pairs.append((i, device(at)))
    return lax.ppermute(value, AXES, pairs)


def across(value):
    return shifted(value, ("core", "core"), 1)


def ring(value, dims):
    came = [value]
    for shift in SHIFTS:
        came.append(shifted(value, dims, shift))
    return jnp.concatenate(came, 0)


def summed_over_cols(value):
    for dim, bit in (("z", 1), ("y", 1), ("y", 2)):
        pairs = []
        for j in range(128):
            at = place(j)
            at[dim] ^= bit
            pairs.append((j, device(at)))
        other = lax.ppermute(value, AXES, pairs)
        value = value + other
    return value


def gather_table(piece, core):
    half = piece.shape[1] // 2
    mine = lax.dynamic_slice_in_dim(piece, core * half, half, 1)
    other = lax.dynamic_slice_in_dim(piece, (1 - core) * half, half, 1)
    came = across(other)
    unit = jnp.where(core == 0, jnp.stack([mine, came]), jnp.stack([came, mine]))
    near = ring(unit[None], ("x", "y"))
    plane = ring(near[None], ("y", "z"))
    last = ("z", "x")
    left = shifted(plane, last, 1)
    right = shifted(plane, last, -1)
    far0 = shifted(left[:2], last, 1)
    far1 = shifted(right[2:], last, -1)
    own = [x.reshape(-1, *unit.shape) for x in (plane, left, right, far0, far1)]
    return own, [across(x) for x in own]


def spot(there, here):
    ahead = (there - here) & 3
    return jnp.where(ahead == 3, 1, jnp.where(ahead == 0, 0, ahead + 1))


def pick_kernel(first_ref, range_ref, index_ref, picked_ref, gram_ref):
    r = range_ref[...].reshape(256, range_ref.shape[2])
    gram_ref[...] = dot(r, r, NT)
    at = lax.broadcasted_iota(jnp.int32, (r.shape[1], index_ref.shape[1]), 0)
    hot = (at == index_ref[...] - first_ref[0]).astype(F32).astype(BF)
    picked_ref[...] = dot(r, hot, NN).T.astype(BF)


def pick(first, second_range, index):
    n = index.shape[1]
    return pl.pallas_call(
        pick_kernel,
        in_specs=[pl.BlockSpec(memory_space=pltpu.SMEM)]
        + [pl.BlockSpec(memory_space=pltpu.VMEM)] * 2,
        out_specs=[pl.BlockSpec(memory_space=pltpu.VMEM)] * 2,
        out_shape=[jax.ShapeDtypeStruct((n, 256), BF), jax.ShapeDtypeStruct((256, 256), F32)],
        cost_estimate=pl.CostEstimate(
            flops=2_000_000_000, bytes_accessed=2_000_000, transcendentals=0
        ),
    )(first, second_range, index)


def piece_table(row_at, col_at, order, slab):
    y, z_lo, z_hi, x = jnp.meshgrid(
        jnp.arange(4), jnp.arange(2), jnp.arange(2), jnp.arange(4), indexing="ij"
    )
    at_x = spot(x, row_at >> 1)
    at_y = spot(y, col_at >> 1)
    at_z = spot(z_hi * 2 + z_lo, (row_at >> 3) * 2 + (col_at & 1))
    first = jnp.where(order == 0, at_x, at_y)
    second = jnp.where(order == 0, at_y, at_z)
    third = jnp.where(order == 0, at_z, at_x)
    late = (third == 3) & (second >= 2)
    array = third + late
    index = (second - 2 * late) * 4 + first
    last = jnp.stack([order, row_at * slab])
    return jnp.concatenate([array.ravel(), index.ravel(), last]).astype(jnp.int32)


def fetch(table, count, rest, pieces, buf, rest_buf, sem, rest_sem, step, slot):
    n = buf.shape[2]
    for j in range(CHUNK):
        at = step * CHUNK + j
        for p in range(n):
            array = table[at * n + p]
            index = table[64 + at * n + p]
            for a, ref in enumerate(pieces):

                @pl.when(array == a)
                def _(ref=ref, p=p, j=j):
                    pltpu.make_async_copy(
                        ref.at[index], buf.at[slot, j, p], sem.at[slot, j]
                    ).start()

    @pl.when(count > 0)
    def _():
        for j in range(CHUNK):
            rest_copy(table, rest, rest_buf, rest_sem, step, slot, j, 0).start()


def rest_copy(table, rest, rest_buf, rest_sem, step, slot, j, group):
    first = pl.multiple_of((2 * (step * CHUNK + j) + table[128]) * STEP, STEP)
    at = pl.multiple_of(group * GROUP, GROUP)
    return pltpu.make_async_copy(
        rest.at[pl.ds(first, STEP), pl.ds(at, GROUP), :],
        rest_buf.at[slot, j],
        rest_sem.at[slot, j],
    )


def accumulate(table, count_ref, head_ref, rest, pieces, sums, bufs, begin):
    fold_ref, gram_ref, extra_ref = sums
    buf, rest_buf, sem, rest_sem = bufs
    step = pl.program_id(0)
    slot = lax.rem(step, 2)
    count = count_ref[0]
    parts = [(j, i) for j in range(CHUNK) for i in range(STEP)]

    @pl.when(step == 0)
    def _():
        begin()
        fetch(table, count, rest, pieces, *bufs, 0, 0)

        @pl.when(count == 0)
        def _():
            rest_buf[...] = jnp.zeros_like(rest_buf)

    @pl.when(step + 1 < pl.num_programs(0))
    def _():
        fetch(table, count, rest, pieces, *bufs, step + 1, 1 - slot)

    for j in range(CHUNK):
        pltpu.make_async_copy(
            pieces[0].at[pl.ds(0, buf.shape[2])], buf.at[slot, j], sem.at[slot, j]
        ).wait()

    @pl.when(count > 0)
    def _():
        for j in range(CHUNK):
            rest_copy(table, rest, rest_buf, rest_sem, step, slot, j, 0).wait()

    def tile():
        return jnp.concatenate([buf[slot, j].reshape(256, STEP * LO) for j in range(CHUNK)], 1)

    def listed():
        return jnp.concatenate([rest_buf[slot, j, i] for j, i in parts], 1)

    t = tile()
    head = jnp.concatenate([head_ref[j, 0, i] for j, i in parts], 1)
    fold_ref[...] += dot(head, t, NT)
    both = dot(jnp.concatenate([t, listed()], 0), t, NT)
    gram_ref[...] += both[:256]
    extra_ref[:GROUP] += both[256:]

    def more(group, carry):
        for j in range(CHUNK):
            copy = rest_copy(table, rest, rest_buf, rest_sem, step, slot, j, group)
            copy.start()
            copy.wait()
        at = pl.multiple_of(group * GROUP, GROUP)
        extra_ref[pl.ds(at, GROUP), :] += dot(listed(), tile(), NT)
        return carry

    lax.fori_loop(1, groups_of(count), more, 0)


def first_kernel(
    table, count_ref, head_ref, rest, p0, p1, p2, p3, p4, fold_ref, gram_ref, extra_ref, *bufs
):
    sums = (fold_ref, gram_ref, extra_ref)

    def begin():
        for ref in sums:
            ref[...] = jnp.zeros_like(ref)

    accumulate(table, count_ref, head_ref, rest, (p0, p1, p2, p3, p4), sums, bufs, begin)


def second_kernel(
    table, count_ref, head_ref, rest, p0, p1, p2, p3, p4, fold_in, gram_in, extra_in,
    second_ref, owner_ref, list_ref, part_ref, gram_ref, fold_ref, extra_ref, *bufs,
):
    def begin():
        fold_ref[...] = fold_in[...]
        gram_ref[...] = gram_in[...]
        extra_ref[...] = extra_in[...]

    sums = (fold_ref, gram_ref, extra_ref)
    accumulate(table, count_ref, head_ref, rest, (p0, p1, p2, p3, p4), sums, bufs, begin)

    @pl.when(pl.program_id(0) == pl.num_programs(0) - 1)
    def _():
        n = owner_ref.shape[1]
        block = lax.broadcasted_iota(jnp.int32, (n, n), 0)
        place = lax.broadcasted_iota(jnp.int32, (n, n), 1)
        own = (block == list_ref[...]) & (place < count_ref[0])
        own = jnp.where(own, 1.0, 0.0).astype(BF)
        head, rest = halves(extra_ref[...])
        fold = fold_ref[...] + (dot(own, head, NN) + dot(own, rest, NN))
        head, rest = halves(second_ref[...].astype(F32) * fold)
        slot = lax.broadcasted_iota(jnp.int32, (part_ref.shape[0], n), 0)
        hot = (slot == owner_ref[...] - table[129]).astype(F32).astype(BF)
        part_ref[...] = dot(hot, head, NN) + dot(hot, rest, NN)


def product(table, count, head, rest, pieces, more, slab):
    n = head.shape[1]
    by_range = head.reshape(HI // STEP // 2, 2, STEP, n, LO)
    ranges = HI // STEP // 2
    any_spec = pl.BlockSpec(memory_space=pl.ANY)
    whole = lambda x: pl.BlockSpec(x.shape, lambda i, *scalars: (0, 0))
    sums = [jax.ShapeDtypeStruct((rows, 256), F32) for rows in (n, 256, n)]
    out = [jax.ShapeDtypeStruct((slab, 256), F32), sums[1]] if more else sums
    scratch = [
        pltpu.VMEM((2, CHUNK, 8, *pieces[0].shape[1:]), BF),
        pltpu.VMEM((2, CHUNK, STEP, GROUP, LO), BF),
        pltpu.SemaphoreType.DMA((2, CHUNK)),
        pltpu.SemaphoreType.DMA((2, CHUNK)),
    ]
    if more:
        scratch = [pltpu.VMEM((n, 256), F32)] * 2 + scratch
    return pl.pallas_call(
        second_kernel if more else first_kernel,
        grid_spec=pltpu.PrefetchScalarGridSpec(
            num_scalar_prefetch=2,
            grid=(ranges // CHUNK,),
            in_specs=[
                pl.BlockSpec(
                    (CHUNK, 1, STEP, n, LO), lambda i, table, count: (i, table[128], 0, 0, 0)
                )
            ]
            + [any_spec] * 6
            + [whole(x) for x in more],
            out_specs=[whole(x) for x in out],
            scratch_shapes=scratch,
        ),
        out_shape=out,
        cost_estimate=pl.CostEstimate(
            flops=15_000_000_000, bytes_accessed=30_000_000, transcendentals=0
        ),
    )(table, count, by_range, rest, *pieces, *more)


def exact(a, b, dims):
    return lax.dot_general(a, b, dims, precision=lax.Precision.HIGHEST, preferred_element_type=F32)


def inverse_kernel(gram_ref, out_ref, ok_ref, a_ref, x_ref, r_ref):
    n = gram_ref.shape[0]
    at_row = lax.broadcasted_iota(jnp.int32, (n, n), 0)
    at_col = lax.broadcasted_iota(jnp.int32, (n, n), 1)
    eye = jnp.where(at_row == at_col, 1.0, 0.0)
    gram = gram_ref[...]
    diagonal = gram * eye
    by_row = lax.rsqrt(jnp.sum(diagonal, 1, keepdims=True))
    by_col = lax.rsqrt(jnp.sum(diagonal, 0, keepdims=True))
    a = gram * by_row * by_col
    bound = jnp.max(jnp.sum(jnp.abs(a), 0, keepdims=True))
    start = jnp.where(bound < 1.9, 1.0, 1.0 / bound)
    a_ref[...] = a
    x_ref[...] = start * eye
    r_ref[...] = eye - start * a

    def size(r):
        return jnp.sqrt(jnp.sum(r * r))

    def unfinished(state):
        i, now, before = state
        stuck = (now < 0.3) & (now > 0.5 * before)
        return (now > TOLERANCE) & (i < 40) & jnp.logical_not(stuck)

    def improve(state):
        i, now, _ = state
        x = x_ref[...] + exact(x_ref[...], r_ref[...], NN)
        r = eye - exact(a_ref[...], x, NN)
        x_ref[...] = x
        r_ref[...] = r
        return i + 1, size(r), now

    last = lax.while_loop(unfinished, improve, (0, size(r_ref[...]), jnp.float32(1e30)))
    x = x_ref[...] + exact(x_ref[...], r_ref[...], NN)
    out_ref[...] = x * by_row * by_col
    ok_ref[0] = jnp.where(last[1] <= TOLERANCE, 1, 0)


def inverse(gram):
    n = gram.shape[0]
    made, ok = pl.pallas_call(
        inverse_kernel,
        out_shape=[jax.ShapeDtypeStruct((n, n), F32), jax.ShapeDtypeStruct((1,), jnp.int32)],
        out_specs=[
            pl.BlockSpec(memory_space=pltpu.VMEM),
            pl.BlockSpec(memory_space=pltpu.SMEM),
        ],
        scratch_shapes=[pltpu.VMEM((n, n), F32)] * 3,
        cost_estimate=pl.CostEstimate(
            flops=5_000_000_000, bytes_accessed=600_000, transcendentals=0
        ),
    )(gram)

    def by_factor():
        factor = jnp.linalg.cholesky(gram)
        return jax.scipy.linalg.cho_solve((factor, True), jnp.eye(n, dtype=F32))

    return lax.cond(ok[0] == 1, lambda: made, by_factor)


def solve_kernel(inverse_ref, spread_ref, out_ref):
    total = spread_ref[0]
    for i in range(1, spread_ref.shape[0]):
        total = total + spread_ref[i]
    out_ref[...] = exact(inverse_ref[...], total, NT).reshape(out_ref.shape)


def solve(inverted, spread):
    n, rows = inverted.shape[0], spread.shape[1]
    return pl.pallas_call(
        solve_kernel,
        out_shape=jax.ShapeDtypeStruct((n // 16, 16, rows), F32),
        cost_estimate=pl.CostEstimate(
            flops=500_000_000, bytes_accessed=1_500_000, transcendentals=0
        ),
    )(inverted, spread)


def per_device(
    block_values,
    block_length,
    block_owner,
    block_second,
    block_third,
    live_blocks,
    second_factor,
    third_factor,
):
    n_rows = lax.axis_size("rows")
    n_cols = lax.axis_size("cols")
    row_at = lax.axis_index("rows")
    col_at = lax.axis_index("cols")
    range_rows = second_factor.shape[0]
    slab = range_rows * n_cols // n_rows

    core = row_at & 1
    own, swapped = gather_table(third_factor.T, core)
    second = jnp.broadcast_to(second_factor.T[None], (n_rows, *second_factor.T.shape))
    second_range = lax.all_to_all(second, "rows", 0, 0, tiled=True)
    picked, local_gram = pick(
        (col_at * range_rows)[None], second_range, block_second[None, :]
    )
    gram_second = summed_over_cols(local_gram)

    hi, lo, v, listed, count = prepare(block_third, block_values, block_length, live_blocks)
    head = build(hi, lo, v)
    rest = build_rest(count, listed, hi, lo, v)
    owner = block_owner[None, :]
    sums = product(piece_table(row_at, col_at, core, slab), count, head, rest, own, (), slab)
    part, gram_third = product(
        piece_table(row_at, col_at, 1 - core, slab),
        count,
        head,
        rest,
        swapped,
        (*sums, picked, owner, listed),
        slab,
    )

    gram = (gram_second / (range_rows * n_cols)) * (
        gram_third / (third_factor.shape[0] * n_cols)
    )
    spread = part.reshape(n_cols, slab // n_cols, -1)
    spread = lax.all_to_all(spread, "cols", 0, 0, tiled=True)
    solved = solve(inverse(gram), spread)
    moved = lax.all_to_all(solved, "rows", 0, 0, tiled=True)
    share = n_rows // n_cols
    moved = moved.reshape(n_cols, share, *solved.shape[1:])
    moved = lax.all_to_all(moved, "cols", 0, 0, tiled=True)
    return moved.transpose(1, 0, 3, 2).reshape(range_rows, solved.shape[1])


def solution(mesh):
    return jax.shard_map(
        per_device,
        mesh=mesh,
        in_specs=(
            P(("rows", "cols"), None),
            P(("rows", "cols")),
            P(("rows", "cols")),
            P(("rows", "cols")),
            P(("rows", "cols"), None),
            P(("rows", "cols")),
            P("cols", "rows"),
            P("cols", "rows"),
        ),
        out_specs=P("cols", "rows"),
        check_vma=False,
    )
```

```python
import functools

import jax
import jax.numpy as jnp
from jax import lax
from jax.experimental import pallas as pl
from jax.experimental.pallas import tpu as pltpu
from jax.sharding import PartitionSpec as P


BF = jnp.bfloat16
F32 = jnp.float32
NT = (((1,), (1,)), ((), ()))
NN = (((1,), (0,)), ((), ()))

LO = 256
HI = 128
NB = 16
PITCH = 140
GROUP = 64
PARTS = (8, 16, 8)
STEP = 8
CHUNK = 2
TOLERANCE = 3e-4
AXES = ("rows", "cols")
SHIFTS = (1, -1, 2)


def dot(a, b, dims):
    return lax.dot_general(a, b, dims, preferred_element_type=F32)


def halves(x):
    head = x.astype(BF)
    return head, (x - head.astype(F32)).astype(BF)


def prepare_kernel(
    live_ref, third_ref, value_ref, length_ref, hi_ref, lo_ref, v_ref, list_ref, count_ref, again
):
    step = pl.program_id(0)
    n, width = third_ref.shape
    third = third_ref[...]
    lane = lax.broadcasted_iota(jnp.int32, (n, width), 1)
    block = lax.broadcasted_iota(jnp.int32, (n, width), 0) + step * n
    across = lax.broadcasted_iota(jnp.int32, (n, width), 0) == lane
    length = jnp.sum(jnp.where(across, length_ref[...].astype(F32), 0.0), 1, keepdims=True)
    live = (lane.astype(F32) < length) & (block < live_ref[0])
    hi_ref[...] = (third >> 8).astype(F32)
    lo_ref[...] = (third & (LO - 1)).astype(F32)
    v_ref[...] = jnp.where(live, value_ref[...].astype(F32), 0.0)
    marked = jnp.where(live, third, (1 << 15) + lane)
    pair = marked[: n // 2] | (marked[n // 2 :] << 16)
    low = jnp.zeros_like(pair)
    high = jnp.zeros_like(pair)
    for shift in range(1, width // 2 + 1):
        differ = pair ^ pltpu.roll(pair, shift, 1)
        low = low | ((differ & 0xFFFF) - 1)
        high = high | (lax.shift_right_logical(differ, 16) - 1)
    same = jnp.concatenate([jnp.where(x < 0, 1.0, 0.0) for x in (low, high)], 0)
    found = jnp.max(same, 1, keepdims=True)
    again[pl.ds(pl.multiple_of(step * n, n), n), :] = jnp.broadcast_to(found, (n, width))

    @pl.when(step == pl.num_programs(0) - 1)
    def _():
        total = again.shape[0]
        flags = again[...]
        row = lax.broadcasted_iota(jnp.int32, (total, total), 0)
        col = lax.broadcasted_iota(jnp.int32, (total, total), 1)
        earlier = jnp.where(col < row, 1.0, 0.0).astype(BF)
        ahead = dot(earlier, flags.astype(BF), NN)
        wide = jnp.concatenate([ahead] * (total // width), 1)
        on = jnp.concatenate([flags] * (total // width), 1)
        mine = (on > 0.5) & (wide == col.astype(F32))
        picked = jnp.sum(jnp.where(mine, row.astype(F32), 0.0), 0, keepdims=True)
        list_ref[...] = picked.astype(jnp.int32)
        count_ref[0] = jnp.sum(flags[:, :1]).astype(jnp.int32)


def prepare(third, values, length, live):
    n, width = third.shape
    rows = 128
    spec = pl.BlockSpec((rows, width), lambda i: (i, 0))
    shape = jax.ShapeDtypeStruct((n, width), F32)
    return pl.pallas_call(
        prepare_kernel,
        grid=(n // rows,),
        in_specs=[
            pl.BlockSpec(memory_space=pltpu.SMEM),
            spec,
            spec,
            pl.BlockSpec((1, rows), lambda i: (0, i)),
        ],
        out_specs=[spec] * 3
        + [pl.BlockSpec((1, n), lambda i: (0, 0)), pl.BlockSpec(memory_space=pltpu.SMEM)],
        out_shape=[shape] * 3
        + [jax.ShapeDtypeStruct((1, n), jnp.int32), jax.ShapeDtypeStruct((1,), jnp.int32)],
        scratch_shapes=[pltpu.VMEM((n, width), F32)],
        cost_estimate=pl.CostEstimate(
            flops=3_000_000_000, bytes_accessed=1_000_000, transcendentals=0
        ),
    )(live, third, values, length[None, :])


def spread_blocks(rows_of, left, right):
    base = lax.broadcasted_iota(jnp.int32, (16, 128), 0)
    iota = [(base + 16 * j).astype(F32).astype(BF) for j in range(LO // 16)]
    one = jnp.ones((16, 128), BF)
    zero = jnp.zeros((16, 128), BF)
    for b in range(NB):
        hi, lo, v = (jnp.broadcast_to(row, (16, 128)).astype(BF) for row in rows_of(b))
        a = jnp.concatenate([jnp.where(hi == iota[j], v, zero) for j in range(HI // 16)], 0)
        c = jnp.concatenate([jnp.where(lo == iota[j], one, zero) for j in range(LO // 16)], 0)
        s = dot(a, c, NT)
        left[b * PITCH : b * PITCH + HI, :] = s[:, :128]
        right[b * PITCH : b * PITCH + HI, :] = s[:, 128:]


def write_blocks(left, right, buf, out_ref, at, sem, value_of):
    quarter = HI // 4
    for q in range(4):

        def some(i, carry, q=q):
            for u in range(16):
                h = q * quarter + i * 16 + u
                blocks = pl.ds(h, NB, stride=PITCH)
                buf[h] = value_of(jnp.concatenate([left[blocks, :], right[blocks, :]], 1))
            return carry

        lax.fori_loop(0, quarter // 16, some, 0)
        rows = pl.ds(q * quarter, quarter)
        pltpu.make_async_copy(buf.at[rows], out_ref.at[rows, pl.ds(at, NB), :], sem).start()


def written(buf, out_ref, sem):
    return pltpu.make_async_copy(buf, out_ref.at[:, pl.ds(0, NB), :], sem)


def build_kernel(first, hi_ref, lo_ref, v_ref, *refs):
    head_ref, left, right, buf, sem = refs[-5:]
    step = pl.program_id(0)
    slot = lax.rem(step, 2)
    spread_blocks(
        lambda b: [ref[b : b + 1, :] for ref in (hi_ref, lo_ref, v_ref)], left, right
    )

    @pl.when(step >= 2)
    def _():
        written(buf.at[slot], head_ref, sem.at[slot]).wait()

    at = pl.multiple_of((first + step) * NB, NB)
    write_blocks(
        left, right, buf.at[slot], head_ref, at, sem.at[slot], lambda x: x.astype(BF)
    )

    @pl.when(step == pl.num_programs(0) - 1)
    def _():
        for i in range(2):
            written(buf.at[i], head_ref, sem.at[i]).wait()


def build(hi, lo, v):
    n = hi.shape[0]
    assert n == NB * sum(PARTS)
    made = ()
    first = 0
    for steps in PARTS:
        spec = pl.BlockSpec((NB, 128), lambda i, first=first: (first + i, 0))
        call = pl.pallas_call(
            functools.partial(build_kernel, first),
            grid=(steps,),
            in_specs=[spec] * 3 + [pl.BlockSpec(memory_space=pl.ANY)] * len(made),
            out_specs=pl.BlockSpec(memory_space=pl.ANY),
            out_shape=jax.ShapeDtypeStruct((HI, n, LO), BF),
            scratch_shapes=[pltpu.VMEM((NB * PITCH, 128), F32)] * 2
            + [pltpu.VMEM((2, HI, NB, LO), BF), pltpu.SemaphoreType.DMA((2,))],
            input_output_aliases={3: 0} if made else {},
            cost_estimate=pl.CostEstimate(
                flops=940_000_000 * steps,
                bytes_accessed=steps * NB * HI * LO * 2,
                transcendentals=0,
            ),
        )
        made = (call(hi, lo, v, *made),)
        first += steps
    return made[0]


def groups_of(count):
    return (count + GROUP - 1) // GROUP


def rest_kernel(count_ref, list_ref, hi_ref, lo_ref, v_ref, rest_ref, left, right, buf, sem):
    count = count_ref[0]

    def some(i, carry):
        def rows_of(b):
            slot = i * NB + b
            block = list_ref[0, slot]
            on = jnp.where(slot < count, 1.0, 0.0).astype(F32)
            hi, lo, v = (ref[pl.ds(block, 1), :] for ref in (hi_ref, lo_ref, v_ref))
            return hi, lo, v * on

        spread_blocks(rows_of, left, right)

        @pl.when(i > 0)
        def _():
            written(buf, rest_ref, sem).wait()

        at = pl.multiple_of(i * NB, NB)
        write_blocks(
            left, right, buf, rest_ref, at, sem, lambda x: (x - x.astype(BF).astype(F32)).astype(BF)
        )
        return carry

    lax.fori_loop(0, groups_of(count) * (GROUP // NB), some, 0)

    @pl.when(count > 0)
    def _():
        written(buf, rest_ref, sem).wait()


def build_rest(count, listed, hi, lo, v):
    n = hi.shape[0]
    return pl.pallas_call(
        rest_kernel,
        in_specs=[pl.BlockSpec(memory_space=pltpu.SMEM)] * 2
        + [pl.BlockSpec(memory_space=pltpu.VMEM)] * 3,
        out_specs=pl.BlockSpec(memory_space=pl.ANY),
        out_shape=jax.ShapeDtypeStruct((HI, n, LO), BF),
        scratch_shapes=[pltpu.VMEM((NB * PITCH, 128), F32)] * 2
        + [pltpu.VMEM((HI, NB, LO), BF), pltpu.SemaphoreType.DMA],
        cost_estimate=pl.CostEstimate(
            flops=6_000_000_000, bytes_accessed=6_000_000, transcendentals=0
        ),
    )(count, listed, hi, lo, v)


def place(i):
    return {
        "x": i // 16 % 4,
        "y": i // 2 % 4,
        "z": i // 64 * 2 + i % 2,
        "core": i // 8 % 2,
    }


def device(at):
    return (((at["z"] // 2 * 4 + at["x"]) * 2 + at["core"]) * 4 + at["y"]) * 2 + at["z"] % 2


def shifted(value, dims, shift):
    pairs = []
    for i in range(128):
        at = place(i)
        dim = dims[at["core"]]
        at[dim] = (at[dim] + shift) % (2 if dim == "core" else 4)
        pairs.append((i, device(at)))
    return lax.ppermute(value, AXES, pairs)


def across(value):
    return shifted(value, ("core", "core"), 1)


def ring(value, dims):
    came = [value]
    for shift in SHIFTS:
        came.append(shifted(value, dims, shift))
    return jnp.concatenate(came, 0)


def summed_over_cols(value):
    for dim, bit in (("z", 1), ("y", 1), ("y", 2)):
        pairs = []
        for j in range(128):
            at = place(j)
            at[dim] ^= bit
            pairs.append((j, device(at)))
        other = lax.ppermute(value, AXES, pairs)
        value = value + other
    return value


def gather_table(piece, core):
    half = piece.shape[1] // 2
    mine = lax.dynamic_slice_in_dim(piece, core * half, half, 1)
    other = lax.dynamic_slice_in_dim(piece, (1 - core) * half, half, 1)
    came = across(other)
    unit = jnp.where(core == 0, jnp.stack([mine, came]), jnp.stack([came, mine]))
    near = ring(unit[None], ("x", "y"))
    plane = ring(near[None], ("y", "z"))
    last = ("z", "x")
    left = shifted(plane, last, 1)
    right = shifted(plane, last, -1)
    far0 = shifted(left[:2], last, 1)
    far1 = shifted(right[2:], last, -1)
    own = [x.reshape(-1, *unit.shape) for x in (plane, left, right, far0, far1)]
    return own, [across(x) for x in own]


def spot(there, here):
    ahead = (there - here) & 3
    return jnp.where(ahead == 3, 1, jnp.where(ahead == 0, 0, ahead + 1))


def pick_kernel(first_ref, range_ref, index_ref, picked_ref, gram_ref):
    r = range_ref[...].reshape(256, range_ref.shape[2])
    gram_ref[...] = dot(r, r, NT)
    at = lax.broadcasted_iota(jnp.int32, (r.shape[1], index_ref.shape[1]), 0)
    hot = (at == index_ref[...] - first_ref[0]).astype(F32).astype(BF)
    picked_ref[...] = dot(r, hot, NN).T.astype(BF)


def pick(first, second_range, index):
    n = index.shape[1]
    return pl.pallas_call(
        pick_kernel,
        in_specs=[pl.BlockSpec(memory_space=pltpu.SMEM)]
        + [pl.BlockSpec(memory_space=pltpu.VMEM)] * 2,
        out_specs=[pl.BlockSpec(memory_space=pltpu.VMEM)] * 2,
        out_shape=[jax.ShapeDtypeStruct((n, 256), BF), jax.ShapeDtypeStruct((256, 256), F32)],
        cost_estimate=pl.CostEstimate(
            flops=2_000_000_000, bytes_accessed=2_000_000, transcendentals=0
        ),
    )(first, second_range, index)


def piece_table(row_at, col_at, order, slab):
    y, z_lo, z_hi, x = jnp.meshgrid(
        jnp.arange(4), jnp.arange(2), jnp.arange(2), jnp.arange(4), indexing="ij"
    )
    at_x = spot(x, row_at >> 1)
    at_y = spot(y, col_at >> 1)
    at_z = spot(z_hi * 2 + z_lo, (row_at >> 3) * 2 + (col_at & 1))
    first = jnp.where(order == 0, at_x, at_y)
    second = jnp.where(order == 0, at_y, at_z)
    third = jnp.where(order == 0, at_z, at_x)
    late = (third == 3) & (second >= 2)
    array = third + late
    index = (second - 2 * late) * 4 + first
    last = jnp.stack([order, row_at * slab])
    return jnp.concatenate([array.ravel(), index.ravel(), last]).astype(jnp.int32)


def fetch(table, count, rest, pieces, buf, rest_buf, sem, rest_sem, step, slot):
    n = buf.shape[2]
    for j in range(CHUNK):
        at = step * CHUNK + j
        for p in range(n):
            array = table[at * n + p]
            index = table[64 + at * n + p]
            for a, ref in enumerate(pieces):

                @pl.when(array == a)
                def _(ref=ref, p=p, j=j):
                    pltpu.make_async_copy(
                        ref.at[index], buf.at[slot, j, p], sem.at[slot, j]
                    ).start()

    @pl.when(count > 0)
    def _():
        for j in range(CHUNK):
            rest_copy(table, rest, rest_buf, rest_sem, step, slot, j, 0).start()


def rest_copy(table, rest, rest_buf, rest_sem, step, slot, j, group):
    first = pl.multiple_of((2 * (step * CHUNK + j) + table[128]) * STEP, STEP)
    at = pl.multiple_of(group * GROUP, GROUP)
    return pltpu.make_async_copy(
        rest.at[pl.ds(first, STEP), pl.ds(at, GROUP), :],
        rest_buf.at[slot, j],
        rest_sem.at[slot, j],
    )


def accumulate(table, count_ref, head_ref, rest, pieces, sums, bufs, begin):
    fold_ref, gram_ref, extra_ref = sums
    buf, rest_buf, sem, rest_sem = bufs
    step = pl.program_id(0)
    slot = lax.rem(step, 2)
    count = count_ref[0]
    parts = [(j, i) for j in range(CHUNK) for i in range(STEP)]

    @pl.when(step == 0)
    def _():
        begin()
        fetch(table, count, rest, pieces, *bufs, 0, 0)

        @pl.when(count == 0)
        def _():
            rest_buf[...] = jnp.zeros_like(rest_buf)

    @pl.when(step + 1 < pl.num_programs(0))
    def _():
        fetch(table, count, rest, pieces, *bufs, step + 1, 1 - slot)

    for j in range(CHUNK):
        pltpu.make_async_copy(
            pieces[0].at[pl.ds(0, buf.shape[2])], buf.at[slot, j], sem.at[slot, j]
        ).wait()

    @pl.when(count > 0)
    def _():
        for j in range(CHUNK):
            rest_copy(table, rest, rest_buf, rest_sem, step, slot, j, 0).wait()

    def tile():
        return jnp.concatenate([buf[slot, j].reshape(256, STEP * LO) for j in range(CHUNK)], 1)

    def listed():
        return jnp.concatenate([rest_buf[slot, j, i] for j, i in parts], 1)

    t = tile()
    head = jnp.concatenate([head_ref[j, 0, i] for j, i in parts], 1)
    fold_ref[...] += dot(head, t, NT)
    both = dot(jnp.concatenate([t, listed()], 0), t, NT)
    gram_ref[...] += both[:256]
    extra_ref[:GROUP] += both[256:]

    def more(group, carry):
        for j in range(CHUNK):
            copy = rest_copy(table, rest, rest_buf, rest_sem, step, slot, j, group)
            copy.start()
            copy.wait()
        at = pl.multiple_of(group * GROUP, GROUP)
        extra_ref[pl.ds(at, GROUP), :] += dot(listed(), tile(), NT)
        return carry

    lax.fori_loop(1, groups_of(count), more, 0)


def first_kernel(
    table, count_ref, head_ref, rest, p0, p1, p2, p3, p4, fold_ref, gram_ref, extra_ref, *bufs
):
    sums = (fold_ref, gram_ref, extra_ref)

    def begin():
        for ref in sums:
            ref[...] = jnp.zeros_like(ref)

    accumulate(table, count_ref, head_ref, rest, (p0, p1, p2, p3, p4), sums, bufs, begin)


def second_kernel(
    table, count_ref, head_ref, rest, p0, p1, p2, p3, p4, fold_in, gram_in, extra_in,
    second_ref, owner_ref, list_ref, part_ref, gram_ref, fold_ref, extra_ref, *bufs,
):
    def begin():
        fold_ref[...] = fold_in[...]
        gram_ref[...] = gram_in[...]
        extra_ref[...] = extra_in[...]

    sums = (fold_ref, gram_ref, extra_ref)
    accumulate(table, count_ref, head_ref, rest, (p0, p1, p2, p3, p4), sums, bufs, begin)

    @pl.when(pl.program_id(0) == pl.num_programs(0) - 1)
    def _():
        n = owner_ref.shape[1]
        block = lax.broadcasted_iota(jnp.int32, (n, n), 0)
        place = lax.broadcasted_iota(jnp.int32, (n, n), 1)
        own = (block == list_ref[...]) & (place < count_ref[0])
        own = jnp.where(own, 1.0, 0.0).astype(BF)
        head, rest = halves(extra_ref[...])
        fold = fold_ref[...] + (dot(own, head, NN) + dot(own, rest, NN))
        head, rest = halves(second_ref[...].astype(F32) * fold)
        slot = lax.broadcasted_iota(jnp.int32, (part_ref.shape[0], n), 0)
        hot = (slot == owner_ref[...] - table[129]).astype(F32).astype(BF)
        part_ref[...] = dot(hot, head, NN) + dot(hot, rest, NN)


def product(table, count, head, rest, pieces, more, slab):
    n = head.shape[1]
    by_range = head.reshape(HI // STEP // 2, 2, STEP, n, LO)
    ranges = HI // STEP // 2
    any_spec = pl.BlockSpec(memory_space=pl.ANY)
    whole = lambda x: pl.BlockSpec(x.shape, lambda i, *scalars: (0, 0))
    sums = [jax.ShapeDtypeStruct((rows, 256), F32) for rows in (n, 256, n)]
    out = [jax.ShapeDtypeStruct((slab, 256), F32), sums[1]] if more else sums
    scratch = [
        pltpu.VMEM((2, CHUNK, 8, *pieces[0].shape[1:]), BF),
        pltpu.VMEM((2, CHUNK, STEP, GROUP, LO), BF),
        pltpu.SemaphoreType.DMA((2, CHUNK)),
        pltpu.SemaphoreType.DMA((2, CHUNK)),
    ]
    if more:
        scratch = [pltpu.VMEM((n, 256), F32)] * 2 + scratch
    return pl.pallas_call(
        second_kernel if more else first_kernel,
        grid_spec=pltpu.PrefetchScalarGridSpec(
            num_scalar_prefetch=2,
            grid=(ranges // CHUNK,),
            in_specs=[
                pl.BlockSpec(
                    (CHUNK, 1, STEP, n, LO), lambda i, table, count: (i, table[128], 0, 0, 0)
                )
            ]
            + [any_spec] * 6
            + [whole(x) for x in more],
            out_specs=[whole(x) for x in out],
            scratch_shapes=scratch,
        ),
        out_shape=out,
        cost_estimate=pl.CostEstimate(
            flops=15_000_000_000, bytes_accessed=30_000_000, transcendentals=0
        ),
    )(table, count, by_range, rest, *pieces, *more)


def exact(a, b, dims):
    return lax.dot_general(a, b, dims, precision=lax.Precision.HIGHEST, preferred_element_type=F32)


def inverse_kernel(gram_ref, out_ref, ok_ref, a_ref, x_ref, r_ref):
    n = gram_ref.shape[0]
    at_row = lax.broadcasted_iota(jnp.int32, (n, n), 0)
    at_col = lax.broadcasted_iota(jnp.int32, (n, n), 1)
    eye = jnp.where(at_row == at_col, 1.0, 0.0)
    gram = gram_ref[...]
    diagonal = gram * eye
    by_row = lax.rsqrt(jnp.sum(diagonal, 1, keepdims=True))
    by_col = lax.rsqrt(jnp.sum(diagonal, 0, keepdims=True))
    a = gram * by_row * by_col
    bound = jnp.max(jnp.sum(jnp.abs(a), 0, keepdims=True))
    start = jnp.where(bound < 1.9, 1.0, 1.0 / bound)
    a_ref[...] = a
    x_ref[...] = start * eye
    r_ref[...] = eye - start * a

    def size(r):
        return jnp.sqrt(jnp.sum(r * r))

    def unfinished(state):
        i, now, before = state
        stuck = (now < 0.3) & (now > 0.5 * before)
        return (now > TOLERANCE) & (i < 40) & jnp.logical_not(stuck)

    def improve(state):
        i, now, _ = state
        x = x_ref[...] + exact(x_ref[...], r_ref[...], NN)
        r = eye - exact(a_ref[...], x, NN)
        x_ref[...] = x
        r_ref[...] = r
        return i + 1, size(r), now

    last = lax.while_loop(unfinished, improve, (0, size(r_ref[...]), jnp.float32(1e30)))
    x = x_ref[...] + exact(x_ref[...], r_ref[...], NN)
    out_ref[...] = x * by_row * by_col
    ok_ref[0] = jnp.where(last[1] <= TOLERANCE, 1, 0)


def inverse(gram):
    n = gram.shape[0]
    made, ok = pl.pallas_call(
        inverse_kernel,
        out_shape=[jax.ShapeDtypeStruct((n, n), F32), jax.ShapeDtypeStruct((1,), jnp.int32)],
        out_specs=[
            pl.BlockSpec(memory_space=pltpu.VMEM),
            pl.BlockSpec(memory_space=pltpu.SMEM),
        ],
        scratch_shapes=[pltpu.VMEM((n, n), F32)] * 3,
        cost_estimate=pl.CostEstimate(
            flops=5_000_000_000, bytes_accessed=600_000, transcendentals=0
        ),
    )(gram)

    def by_factor():
        factor = jnp.linalg.cholesky(gram)
        return jax.scipy.linalg.cho_solve((factor, True), jnp.eye(n, dtype=F32))

    return lax.cond(ok[0] == 1, lambda: made, by_factor)


def solve_kernel(inverse_ref, spread_ref, out_ref):
    total = spread_ref[0]
    for i in range(1, spread_ref.shape[0]):
        total = total + spread_ref[i]
    out_ref[...] = exact(inverse_ref[...], total, NT).reshape(out_ref.shape)


def solve(inverted, spread):
    n, rows = inverted.shape[0], spread.shape[1]
    return pl.pallas_call(
        solve_kernel,
        out_shape=jax.ShapeDtypeStruct((n // 16, 16, rows), F32),
        cost_estimate=pl.CostEstimate(
            flops=500_000_000, bytes_accessed=1_500_000, transcendentals=0
        ),
    )(inverted, spread)


def per_device(
    block_values,
    block_length,
    block_owner,
    block_second,
    block_third,
    live_blocks,
    second_factor,
    third_factor,
):
    n_rows = lax.axis_size("rows")
    n_cols = lax.axis_size("cols")
    row_at = lax.axis_index("rows")
    col_at = lax.axis_index("cols")
    range_rows = second_factor.shape[0]
    slab = range_rows * n_cols // n_rows

    core = row_at & 1
    own, swapped = gather_table(third_factor.T, core)
    second = jnp.broadcast_to(second_factor.T[None], (n_rows, *second_factor.T.shape))
    second_range = lax.all_to_all(second, "rows", 0, 0, tiled=True)
    picked, local_gram = pick(
        (col_at * range_rows)[None], second_range, block_second[None, :]
    )
    gram_second = summed_over_cols(local_gram)

    hi, lo, v, listed, count = prepare(block_third, block_values, block_length, live_blocks)
    head = build(hi, lo, v)
    rest = build_rest(count, listed, hi, lo, v)
    owner = block_owner[None, :]
    sums = product(piece_table(row_at, col_at, core, slab), count, head, rest, own, (), slab)
    part, gram_third = product(
        piece_table(row_at, col_at, 1 - core, slab),
        count,
        head,
        rest,
        swapped,
        (*sums, picked, owner, listed),
        slab,
    )

    gram = (gram_second / (range_rows * n_cols)) * (
        gram_third / (third_factor.shape[0] * n_cols)
    )
    spread = part.reshape(n_cols, slab // n_cols, -1)
    spread = lax.all_to_all(spread, "cols", 0, 0, tiled=True)
    solved = solve(inverse(gram), spread)
    moved = lax.all_to_all(solved, "rows", 0, 0, tiled=True)
    share = n_rows // n_cols
    moved = moved.reshape(n_cols, share, *solved.shape[1:])
    moved = lax.all_to_all(moved, "cols", 0, 0, tiled=True)
    return moved.transpose(1, 0, 3, 2).reshape(range_rows, solved.shape[1])


def solution(mesh):
    return jax.shard_map(
        per_device,
        mesh=mesh,
        in_specs=(
            P(("rows", "cols"), None),
            P(("rows", "cols")),
            P(("rows", "cols")),
            P(("rows", "cols")),
            P(("rows", "cols"), None),
            P(("rows", "cols")),
            P("cols", "rows"),
            P("cols", "rows"),
        ),
        out_specs=P("cols", "rows"),
        check_vma=False,
    )
```
